1024 devices in a mesh: sfc: 256 (over x, z, core), lvl: 4 (over y).
Axes of the slice: x: 4, y: 4, z: 32, core: 2. Of those that a mesh axis runs over, the one named last changes fastest.
Arguments:
- right_side: float32 [524288, 128], P(('sfc', 'lvl')), may hold values from -48 to 48
- cell_coef: float32 [524288], P(('sfc', 'lvl')), may hold values from 4 to 16
- fine_count: int32 [1024], replicated, may hold values from 256 to 512, as said below
- cell_matrix: float32 [128, 128], replicated, may hold values from -0.5 to 0.5
- face_near: float32 [128, 128], replicated, may hold values from -0.5 to 0.5
- face_far: float32 [128, 128], replicated, may hold values from -0.5 to 0.5
- prolong: float32 [8, 128, 128], replicated, may hold values from -0.5 to 0.5
Outputs:
- solution: float32 [524288, 128], P(('sfc', 'lvl'))
The draws below stay inside these ranges and needn't reach their ends.
Inputs may be any that keep to these rules, and one draw needn't show every extreme that they name: `fine_count`: each device's count is a multiple of 8 and at least 256; exactly one device holds 512, every other at most 504.
All inputs are finite; a program needn't handle non-finite values.
Results may differ from the reference program's by a relative error of at most 0.000051.
Values sent between devices are 32-bit elements; how exact they have to be, the bound alone decides.
A program may use at most 32 MiB of HBM per device.

```python
import math
import jax
import jax.numpy as jnp
from jax import lax

V = 128
CAP = 512
DEG = 3
W = 32
WC = 32
SLOTS = 524288
DEVICES = 1024


def draw_fine_count(key, part):
    key_values, key_top = jax.random.split(jax.random.fold_in(key, 17))
    counts = jax.random.randint(key_values, (DEVICES,), CAP // 16, CAP // 8) * 8
    fullest = jax.random.randint(key_top, (), 0, DEVICES)
    return counts.at[fullest].set(CAP).astype(jnp.int32)


def shard_levels(own_key, dims, pieces, low, high):
    gain = 1.0
    for axis_at, shards_of in pieces:
        steps = jax.random.uniform(jax.random.fold_in(jax.random.fold_in(own_key, 6), axis_at), (shards_of,), jnp.float32, low / len(pieces), high / len(pieces))
        gain = gain * jnp.repeat(jnp.exp(steps), dims[axis_at] // shards_of).reshape((-1,) + (1,) * (len(dims) - 1 - axis_at))
    return gain


def gaussian(own_key, extent, spread, limit, shards=(), held_as=jnp.bfloat16):
    values = jax.random.normal(own_key, extent, jnp.float32) * spread
    if len(shards) > 0:
        values = shard_levels(own_key, extent, shards, -0.22, 0.18) * values
    return jnp.clip(values, min=-limit, max=limit).astype(held_as)


def setup_inputs(seed: int = 0) -> dict:
    arg_keys = jax.random.split(jax.random.key(seed), 8)
    right_side = gaussian(arg_keys[0], (SLOTS, V), 8.0, 48.0, ((0, 1024),), jnp.float32)
    cell_coef = jnp.clip(jnp.exp(math.log(16.0) - 1.3862944 * jax.random.uniform(arg_keys[1], (SLOTS,), jnp.float32) ** shard_levels(arg_keys[1], (SLOTS,), ((0, 1024),), -0.2, 0.2)), 4.0, 16.0)
    fine_count = draw_fine_count(jax.random.fold_in(arg_keys[7], 71), 0)
    cell_matrix = gaussian(arg_keys[3], (V, V), V ** -0.5, 0.5, (), jnp.float32)
    face_near = gaussian(arg_keys[4], (V, V), V ** -0.5, 0.5, (), jnp.float32)
    face_far = gaussian(arg_keys[5], (V, V), V ** -0.5, 0.5, (), jnp.float32)
    prolong = gaussian(arg_keys[6], (8, V, V), V ** -0.5, 0.5, (), jnp.float32)
    return {"right_side": right_side, "cell_coef": cell_coef, "fine_count": fine_count, "cell_matrix": cell_matrix, "face_near": face_near, "face_far": face_far, "prolong": prolong}


def shifted_dot(field, matrix):
    return jnp.dot(field, matrix, precision=lax.Precision.HIGHEST, preferred_element_type=jnp.float32)


def chain_apply(field, chain_coef, is_live, stride, cell_matrix, face_near, face_far):
    zero_one = jnp.zeros((1, field.shape[1]), jnp.float32)
    zero_far = jnp.zeros((stride, field.shape[1]), jnp.float32)
    next_one = jnp.concatenate([field[1:], zero_one], 0)
    prev_one = jnp.concatenate([zero_one, field[:-1]], 0)
    next_far = jnp.concatenate([field[stride:], zero_far], 0)
    prev_far = jnp.concatenate([zero_far, field[:-stride]], 0)
    result = chain_coef[:, None] * field + shifted_dot(field, cell_matrix)
    result = result - shifted_dot(next_one, face_near) - shifted_dot(prev_one, face_near.T)
    result = result - shifted_dot(next_far, face_far) - shifted_dot(prev_far, face_far.T)
    return jnp.where(is_live[:, None], result, 0.0)


def jacobi_scale(chain_coef, is_live, cell_diag):
    safe_coef = jnp.where(is_live, chain_coef, 16.0)
    return jnp.where(is_live[:, None], 1.0 / (safe_coef[:, None] + cell_diag[None, :]), 0.0)


def chebyshev(apply_fn, jacobi, source, start):
    center = 1.025
    radius = 0.775
    sigma_ratio = center / radius
    if start is None:
        residual = source
    else:
        residual = source - apply_fn(start)
    update = jacobi * residual / center
    iterate = update if start is None else start + update
    weight_prev = 1.0 / sigma_ratio
    for repeat in range(DEG - 1):
        weight_next = 1.0 / (2.0 * sigma_ratio - weight_prev)
        residual = source - apply_fn(iterate)
        update = weight_next * weight_prev * update + (2.0 * weight_next / radius) * jacobi * residual
        iterate = iterate + update
        weight_prev = weight_next
    return iterate


def reference(right_side, cell_coef, fine_count, cell_matrix, face_near, face_far, prolong):
    total_slots = right_side.shape[0]
    values = right_side.shape[1]
    slot_index = jnp.arange(total_slots, dtype=jnp.int32)
    owner = (slot_index // CAP).astype(jnp.int32)
    is_slot_live = (slot_index % CAP) < fine_count[owner]
    chain_rank = (jnp.cumsum(is_slot_live.astype(jnp.int32)) - 1).astype(jnp.int32)
    chain_slot = jnp.where(is_slot_live, chain_rank, total_slots).astype(jnp.int32)
    live_total = jnp.sum(fine_count)
    source = jnp.zeros_like(right_side).at[chain_slot].set(right_side, mode="drop")
    chain_coef = jnp.zeros_like(cell_coef).at[chain_slot].set(cell_coef, mode="drop")
    is_live = slot_index < live_total
    cell_diag = jnp.diagonal(cell_matrix)
    jacobi = jacobi_scale(chain_coef, is_live, cell_diag)

    def fine_apply(field):
        return chain_apply(field, chain_coef, is_live, W, cell_matrix, face_near, face_far)

    iterate = chebyshev(fine_apply, jacobi, source, None)
    residual = source - fine_apply(iterate)
    restrict_map = jnp.transpose(prolong, (0, 2, 1)).reshape(8 * values, values)
    coarse_source = jnp.dot(residual.reshape(total_slots // 8, 8 * values), restrict_map, precision=lax.Precision.HIGHEST, preferred_element_type=jnp.float32)
    coarse_coef = jnp.mean(chain_coef.reshape(total_slots // 8, 8), axis=1)
    coarse_index = jnp.arange(total_slots // 8, dtype=jnp.int32)
    is_coarse = coarse_index < live_total // 8
    coarse_jacobi = jacobi_scale(coarse_coef, is_coarse, cell_diag)

    def coarse_apply(field):
        return chain_apply(field, coarse_coef, is_coarse, WC, cell_matrix, face_near, face_far)

    correction = chebyshev(coarse_apply, coarse_jacobi, coarse_source, None)
    prolong_map = jnp.transpose(prolong, (1, 0, 2)).reshape(values, 8 * values)
    iterate = iterate + jnp.dot(correction, prolong_map, precision=lax.Precision.HIGHEST, preferred_element_type=jnp.float32).reshape(total_slots, values)
    iterate = chebyshev(fine_apply, jacobi, source, iterate)
    gathered = iterate[jnp.maximum(chain_rank, 0)]
    return jnp.where(is_slot_live[:, None], gathered, 0.0)
```

```python
import functools

import jax
import jax.numpy as jnp
from jax import lax
from jax.experimental import pallas as pl
from jax.experimental.pallas import tpu as pltpu
from jax.sharding import PartitionSpec as P

DEG = 3
CENTER = 1.025
RADIUS = 0.775
STEPS = (1, -1, 2, -2, 3, -3)
F32 = jnp.float32
BF16 = jnp.bfloat16


def weights_of():
    ratio = CENTER / RADIUS
    prev = 1.0 / ratio
    pairs = []
    for _ in range(DEG - 1):
        new = 1.0 / (2.0 * ratio - prev)
        pairs.append((new * prev, 2.0 * new / RADIUS))
        prev = new
    return pairs


def split(x):
    high = x.astype(BF16)
    low = (x - high.astype(F32)).astype(BF16)
    return high, low


def rows_of(start, size):
    return start + lax.broadcasted_iota(jnp.int32, (size, 128), 0)


def columns(row):
    return jnp.transpose(jnp.broadcast_to(row, (128, 128)))


def cycle(
    n, lanes, cap,
    counts_hbm, b_hbm, coef_hbm, cell_hbm, near_hbm, far_hbm, prolong_hbm,
    out_ref,
    counts, b_own, coef, cell, near, far, prolong,
    tail, ghost_low, ghost_high, meta, meta_in,
    a_left, a_high, wide_b, wide_a, wide_j, x, d, y, res,
    main_w, low_w, rest_w, rest_low, pro_w, pro_low,
    c_own, c_tail, c_coef, l1, l2, l3, r1, r2, r3, k1, k2, k3, q1, q2, q3,
    c_b, c_a, c_j, c_x, c_d,
    local_sem, b_send, b_recv, m_send, m_recv, c_send, c_recv,
):
    stride = cap // 16
    depth = 5 * stride
    total = cap + 2 * depth
    c_cap = cap // 8
    base = c_cap + 16
    c_total = base + c_cap + base
    half = cap // 2
    me = lax.axis_index("sfc") * lanes + lax.axis_index("lvl")

    def at(step):
        return lax.rem(me + (step + n), n)

    def device(step):
        t = at(step)
        return (lax.div(t, lanes), lax.rem(t, lanes))

    barrier = pltpu.get_barrier_semaphore()
    for s in STEPS:
        pl.semaphore_signal(
            barrier, inc=1, device_id=device(s), device_id_type=pl.DeviceIdType.MESH
        )
    loads = [
        pltpu.make_async_copy(src, dst, local_sem.at[i])
        for i, (src, dst) in enumerate(
            [
                (counts_hbm, counts), (coef_hbm, coef), (b_hbm, b_own), (cell_hbm, cell),
                (near_hbm, near), (far_hbm, far), (prolong_hbm, prolong),
            ]
        )
    ]
    for c in loads:
        c.start()

    def remote(src, dst, send, recv, slot):
        return pltpu.make_async_remote_copy(
            src_ref=src, dst_ref=dst, send_sem=send.at[slot], recv_sem=recv.at[slot],
            device_id=device(STEPS[slot]), device_id_type=pl.DeviceIdType.MESH,
        )

    loads[0].wait()
    loads[1].wait()
    def count(t):
        return jnp.minimum(jnp.maximum(counts[t], half), cap)

    live = count(me)
    c_live = lax.div(live, 8)
    for i in range(cap // 128):
        wide_a[pl.ds(depth + 128 * i, 128), :] = columns(coef[pl.ds(i, 1), :])
    mean = wide_a[pl.ds(depth, c_cap, stride=8), :]
    for c in range(1, 8):
        mean = mean + wide_a[pl.ds(depth + c, c_cap, stride=8), :]
    mean = mean * 0.125
    c_coef[pl.ds(0, c_cap), :] = jnp.zeros((c_cap, 128), F32)
    c_coef[pl.ds(c_cap, c_cap), :] = mean
    c_own[pl.ds(0, c_cap), :] = jnp.zeros((c_cap, 128), F32)
    both = jnp.concatenate([mean, c_coef[pl.ds(c_live, c_cap), :]], 0)
    meta[pl.ds(0, 4), :] = coef[...]
    meta[pl.ds(4, 4), :] = jnp.transpose(both)[0:4, :]

    loads[2].wait()
    tail[...] = b_own[pl.ds(8 * (c_live - depth // 8), depth), :]
    pl.semaphore_wait(barrier, len(STEPS))
    halo = [
        remote(tail, ghost_low, b_send, b_recv, 0),
        remote(b_own.at[pl.ds(0, depth)], ghost_high.at[pl.ds(half, depth)], b_send, b_recv, 1),
    ]
    metas = [
        remote(meta, meta_in.at[i], m_send, m_recv, i) for i in range(len(STEPS))
    ]
    metas[0].start()
    metas[1].start()
    for c in halo:
        c.start()
    for c in metas[2:]:
        c.start()

    for c in loads[3:6]:
        c.wait()
    near_m = near[...]
    far_m = far[...]
    cell_m = cell[...]
    blocks = [cell_m, -near_m, -jnp.transpose(near_m), -far_m, -jnp.transpose(far_m)]
    for i, m in enumerate(blocks):
        high, low = split(m)
        main_w[pl.ds(0, 128), pl.ds(128 * i, 128)] = high
        main_w[pl.ds(128, 128), pl.ds(128 * i, 128)] = high
        low_w[:, pl.ds(128 * i, 128)] = low
    eye = lax.broadcasted_iota(jnp.int32, (128, 128), 0) == lax.broadcasted_iota(
        jnp.int32, (128, 128), 1
    )
    diag = jnp.sum(jnp.where(eye, cell_m, 0.0), axis=0, keepdims=True)
    loads[6].wait()
    for i in range(8):
        m = prolong[i]
        high, low = split(m)
        pro_w[pl.ds(0, 128), pl.ds(128 * i, 128)] = high
        pro_w[pl.ds(128, 128), pl.ds(128 * i, 128)] = high
        pro_low[:, pl.ds(128 * i, 128)] = low
        high, low = split(jnp.transpose(m))
        rest_w[pl.ds(256 * i, 128), :] = high
        rest_w[pl.ds(256 * i + 128, 128), :] = high
        rest_low[pl.ds(128 * i, 128), :] = low
    y[:, pl.ds(0, stride), :] = jnp.zeros((5, stride, 128), F32)
    y[:, pl.ds(stride + total, stride), :] = jnp.zeros((5, stride, 128), F32)

    for c in metas:
        c.wait_recv()
    for i in range(cap // 128):
        a_left[pl.ds(128 * i, 128), :] = columns(meta_in[0, pl.ds(i, 1), :])
    for i in range(2):
        a_high[pl.ds(half + 128 * i, 128), :] = columns(meta_in[1, pl.ds(i, 1), :])
    for i, (ref, at_row, first, size) in enumerate(
        [
            (k1, 16, 128 - c_cap, c_cap), (q1, 32, 0, c_cap),
            (k2, 0, 128 - 48, 48), (q2, 64, 0, 48),
            (k3, 0, 128 - 16, 16), (q3, 96, 0, 16),
        ]
    ):
        ref[pl.ds(at_row, size), :] = columns(meta_in[i, pl.ds(4, 1), :])[first : first + size]

    has_prev = me > 0
    has_next = me < n - 1
    left_live = count(at(-1))
    low_limit = jnp.where(has_prev, 0, depth)
    high_limit = depth + live + jnp.where(has_next, depth, 0)
    shift = 8 * (cap // 8 - c_live)
    n1 = lax.div(left_live, 8)
    a_low = a_left[pl.ds(8 * (n1 - depth // 8), depth), :]
    own_a = wide_a[pl.ds(depth + half, half), :]
    more_a = a_high[pl.ds(shift, cap + depth - half), :]
    index = rows_of(depth + half, cap + depth - half)
    inside = index < depth + live
    wide_a[pl.ds(0, depth), :] = jnp.where(rows_of(0, depth) >= low_limit, a_low, 0.0)
    padded_a = jnp.concatenate([own_a, jnp.zeros((depth, 128), F32)], 0)
    wide_a[pl.ds(depth + half, cap + depth - half), :] = jnp.where(
        index < high_limit, jnp.where(inside, padded_a, more_a), 0.0
    )
    all_rows = rows_of(0, total)
    is_live = (all_rows >= low_limit) & (all_rows < high_limit)
    wide_j[...] = jnp.where(is_live, 1.0 / (jnp.where(is_live, wide_a[...], 16.0) + diag), 0.0)

    for c in halo:
        c.wait_recv()
    wide_b[pl.ds(0, depth), :] = jnp.where(
        rows_of(0, depth) >= low_limit, ghost_low[...], 0.0
    )
    wide_b[pl.ds(depth, half), :] = b_own[pl.ds(0, half), :]
    padded_b = jnp.concatenate(
        [b_own[pl.ds(half, half), :], jnp.zeros((depth, 128), F32)], 0
    )
    more_b = ghost_high[pl.ds(shift, cap + depth - half), :]
    wide_b[pl.ds(depth + half, cap + depth - half), :] = jnp.where(
        index < high_limit, jnp.where(inside, padded_b, more_b), 0.0
    )

    def products(field, low, high):
        first, size = low - stride, high - low + 2 * stride
        hi, lo = split(field[pl.ds(first, size), :])
        pair = jnp.concatenate([hi, lo], 1)
        for start in range(0, 640, 256):
            width = min(256, 640 - start)
            part = jnp.dot(
                pair, main_w[:, pl.ds(start, width)], preferred_element_type=F32
            ) + jnp.dot(hi, low_w[:, pl.ds(start, width)], preferred_element_type=F32)
            for k in range(width // 128):
                y[start // 128 + k, pl.ds(stride + first, size), :] = part[
                    :, 128 * k : 128 * k + 128
                ]

    def applied(field, coefs, low, high):
        size = high - low
        row = stride + low
        return (
            coefs[pl.ds(low, size), :] * field[pl.ds(low, size), :]
            + y[0, pl.ds(row, size), :]
            + y[1, pl.ds(row + 1, size), :]
            + y[2, pl.ds(row - 1, size), :]
            + y[3, pl.ds(row + stride, size), :]
            + y[4, pl.ds(row - stride, size), :]
        )

    def residual(field, coefs, source, low, high):
        products(field, low, high)
        return source[pl.ds(low, high - low), :] - applied(field, coefs, low, high)

    def improve(field, update, coefs, scale, source, low, high, keep, gain):
        rows = pl.ds(low, high - low)
        r = residual(field, coefs, source, low, high)
        step = gain * scale[rows, :] * r
        if keep is not None:
            step = keep * update[rows, :] + step
        update[rows, :] = step
        field[rows, :] = field[rows, :] + step

    pairs = weights_of()
    first = wide_j[...] * wide_b[...] * (1.0 / CENTER)
    x[...] = first
    d[...] = first
    low, high = stride, total - stride
    for keep, gain in pairs:
        improve(x, d, wide_a, wide_j, wide_b, low, high, keep, gain)
        low, high = low + stride, high - stride
    res[...] = residual(x, wide_a, wide_b, depth, depth + cap)

    acc = jnp.zeros((c_cap, 128), F32)
    for i in range(8):
        hi, lo = split(res[pl.ds(i, c_cap, stride=8), :])
        acc = acc + jnp.dot(
            jnp.concatenate([hi, lo], 1), rest_w[pl.ds(256 * i, 256), :],
            preferred_element_type=F32,
        )
        acc = acc + jnp.dot(hi, rest_low[pl.ds(128 * i, 128), :], preferred_element_type=F32)
    c_own[pl.ds(c_cap, c_cap), :] = acc
    c_tail[...] = c_own[pl.ds(c_live, c_cap), :]
    coarse = [
        remote(c_tail, l1.at[pl.ds(16, c_cap)], c_send, c_recv, 0),
        remote(c_own.at[pl.ds(c_cap, c_cap)], r1.at[pl.ds(32, c_cap)], c_send, c_recv, 1),
        remote(c_tail.at[pl.ds(c_cap - 48, 48)], l2.at[pl.ds(0, 48)], c_send, c_recv, 2),
        remote(c_own.at[pl.ds(c_cap, 48)], r2.at[pl.ds(64, 48)], c_send, c_recv, 3),
        remote(c_tail.at[pl.ds(c_cap - 16, 16)], l3.at[pl.ds(0, 16)], c_send, c_recv, 4),
        remote(c_own.at[pl.ds(c_cap, 16)], r3.at[pl.ds(96, 16)], c_send, c_recv, 5),
    ]
    for c in coarse:
        c.start()

    n2 = lax.div(count(at(-2)), 8)
    p1 = lax.div(count(at(1)), 8)
    p2 = lax.div(count(at(2)), 8)
    e2 = base - n1
    e3 = e2 - n2
    s1 = base + c_live
    s2 = s1 + p1
    s3 = s2 + p2
    c_low = jnp.where(
        me >= 3, e3 - 16, jnp.where(me == 2, e3, jnp.where(me == 1, e2, base))
    )
    c_high = jnp.where(
        me + 3 < n, s3 + 16, jnp.where(me + 3 == n, s3, jnp.where(me + 2 == n, s2, s1))
    )

    def gathered(target, own, b1, b2, b3, a1, a2, a3):
        r = rows_of(0, base)
        v2 = jnp.concatenate([b2[pl.ds(48 - e2, 48), :], jnp.zeros((base - 48, 128), F32)], 0)
        v3 = jnp.concatenate([b3[pl.ds(16 - e3, 16), :], jnp.zeros((base - 16, 128), F32)], 0)
        value = jnp.where(r >= e2, b1[...], jnp.where(r >= e3, v2, v3))
        target[pl.ds(0, base), :] = jnp.where(r >= c_low, value, 0.0)
        r = rows_of(base, c_cap + base)
        v0 = jnp.concatenate([own, jnp.zeros((base, 128), F32)], 0)
        v1 = jnp.concatenate([jnp.zeros((32, 128), F32), a1[pl.ds(c_cap - c_live, 112), :]], 0)
        v2 = jnp.concatenate([jnp.zeros((64, 128), F32), a2[pl.ds(208 - s2, 80), :]], 0)
        v3 = jnp.concatenate([jnp.zeros((96, 128), F32), a3[pl.ds(272 - s3, 48), :]], 0)
        value = jnp.where(
            r < s1, v0, jnp.where(r < s2, v1, jnp.where(r < s3, v2, v3))
        )
        target[pl.ds(base, c_cap + base), :] = jnp.where(r < c_high, value, 0.0)

    gathered(c_a, mean, k1, k2, k3, q1, q2, q3)
    r = rows_of(0, c_total)
    c_live_rows = (r >= c_low) & (r < c_high)
    c_j[...] = jnp.where(
        c_live_rows, 1.0 / (jnp.where(c_live_rows, c_a[...], 16.0) + diag), 0.0
    )
    for c in coarse:
        c.wait_recv()
    gathered(c_b, acc, l1, l2, l3, r1, r2, r3)
    first = c_j[...] * c_b[...] * (1.0 / CENTER)
    c_x[...] = first
    c_d[...] = first
    for i, (keep, gain) in enumerate(pairs):
        low = stride * (i + 1)
        improve(c_x, c_d, c_a, c_j, c_b, low, c_total - low, keep, gain)

    rows = c_cap + 32
    hi, lo = split(c_x[pl.ds(base - 16, rows), :])
    pair = jnp.concatenate([hi, lo], 1)
    for start in range(0, 1024, 256):
        part = jnp.dot(
            pair, pro_w[:, pl.ds(start, 256)], preferred_element_type=F32
        ) + jnp.dot(hi, pro_low[:, pl.ds(start, 256)], preferred_element_type=F32)
        for k in range(2):
            where = pl.ds(depth - 128 + start // 128 + k, rows, stride=8)
            x[where, :] = x[where, :] + part[:, 128 * k : 128 * k + 128]

    low, high = depth - 2 * stride, depth + cap + 2 * stride
    improve(x, d, wide_a, wide_j, wide_b, low, high, None, 1.0 / CENTER)
    for keep, gain in pairs:
        low, high = low + stride, high - stride
        improve(x, d, wide_a, wide_j, wide_b, low, high, keep, gain)
    out_ref[...] = jnp.where(rows_of(0, cap) < live, x[pl.ds(depth, cap), :], 0.0)
    for c in halo + metas + coarse:
        c.wait_send()


def shards(n, lanes, right_side, cell_coef, fine_count, cell_matrix, face_near, face_far, prolong):
    cap = right_side.shape[0]
    stride = cap // 16
    depth = 5 * stride
    total = cap + 2 * depth
    c_cap = cap // 8
    base = c_cap + 16
    c_total = 2 * base + c_cap
    half = cap // 2

    def vmem(*shape, dtype=F32):
        return pltpu.VMEM(shape, dtype)

    scratch = [
        pltpu.SMEM(fine_count.shape, jnp.int32), vmem(cap, 128), vmem(4, 128),
        vmem(128, 128), vmem(128, 128), vmem(128, 128), vmem(8, 128, 128),
        vmem(depth, 128), vmem(depth, 128), vmem(cap + depth, 128), vmem(8, 128),
        vmem(6, 8, 128),
        vmem(cap, 128), vmem(cap + depth, 128), vmem(total, 128), vmem(total, 128),
        vmem(total, 128), vmem(total, 128), vmem(total, 128),
        vmem(5, total + 2 * stride, 128), vmem(cap, 128),
        vmem(256, 640, dtype=BF16), vmem(128, 640, dtype=BF16),
        vmem(2048, 128, dtype=BF16), vmem(1024, 128, dtype=BF16),
        vmem(256, 1024, dtype=BF16), vmem(128, 1024, dtype=BF16),
        vmem(2 * c_cap, 128), vmem(c_cap, 128), vmem(2 * c_cap, 128),
    ]
    for _ in range(2):
        scratch += [vmem(base, 128)] * 3 + [vmem(base + c_cap, 128)] * 3
    scratch += [vmem(c_total, 128)] * 5
    dma = pltpu.SemaphoreType.DMA
    scratch += [dma((7,)), dma((2,)), dma((2,)), dma((6,)), dma((6,)), dma((6,)), dma((6,))]
    return pl.pallas_call(
        functools.partial(cycle, n, lanes, cap),
        out_shape=jax.ShapeDtypeStruct(right_side.shape, F32),
        in_specs=[pl.BlockSpec(memory_space=pl.ANY)] * 7,
        out_specs=pl.BlockSpec(memory_space=pltpu.VMEM),
        scratch_shapes=scratch,
        compiler_params=pltpu.CompilerParams(collective_id=0, has_side_effects=True),
        name="cycle",
    )(
        fine_count, right_side, cell_coef.reshape(4, 128), cell_matrix, face_near, face_far,
        prolong,
    )


def solution(mesh):
    placed = (P(("sfc", "lvl"), None), P(("sfc", "lvl")), P(), P(), P(), P(), P())
    lanes = mesh.shape["lvl"]
    n = mesh.shape["sfc"] * lanes
    return jax.shard_map(
        functools.partial(shards, n, lanes),
        mesh=mesh, in_specs=placed, out_specs=P(("sfc", "lvl"), None), check_vma=False,
    )
```

```python
import functools

import jax
import jax.numpy as jnp
from jax import lax
from jax.experimental import pallas as pl
from jax.experimental.pallas import tpu as pltpu
from jax.sharding import PartitionSpec as P

DEG = 3
CENTER = 1.025
RADIUS = 0.775
STEPS = (1, -1, 2, -2, 3, -3)
F32 = jnp.float32
BF16 = jnp.bfloat16


def weights_of():
    ratio = CENTER / RADIUS
    prev = 1.0 / ratio
    pairs = []
    for _ in range(DEG - 1):
        new = 1.0 / (2.0 * ratio - prev)
        pairs.append((new * prev, 2.0 * new / RADIUS))
        prev = new
    return pairs


def split(x):
    high = x.astype(BF16)
    low = (x - high.astype(F32)).astype(BF16)
    return high, low


def rows_of(start, size):
    return start + lax.broadcasted_iota(jnp.int32, (size, 128), 0)


def columns(row):
    return jnp.transpose(jnp.broadcast_to(row, (128, 128)))


def cycle(
    n, lanes, cap,
    counts_hbm, b_hbm, coef_hbm, cell_hbm, near_hbm, far_hbm, prolong_hbm,
    out_ref,
    counts, b_own, coef, cell, near, far, prolong,
    tail, ghost_low, ghost_high, meta, meta_in,
    a_left, a_high, wide_b, wide_a, wide_j, x, d, y, res,
    main_w, low_w, rest_w, rest_low, pro_w, pro_low,
    c_own, c_tail, c_coef, l1, l2, l3, r1, r2, r3, k1, k2, k3, q1, q2, q3,
    c_b, c_a, c_j, c_x, c_d,
    x_tail, x_head, x_low, x_high,
    local_sem, b_send, b_recv, m_send, m_recv, c_send, c_recv, x_send, x_recv,
):
    stride = cap // 16
    depth = 3 * stride
    total = cap + 2 * depth
    c_cap = cap // 8
    base = c_cap + 16
    c_total = base + c_cap + base
    half = cap // 2
    me = lax.axis_index("sfc") * lanes + lax.axis_index("lvl")

    def at(step):
        return lax.rem(me + (step + n), n)

    def device(step):
        t = at(step)
        return (lax.div(t, lanes), lax.rem(t, lanes))

    barrier = pltpu.get_barrier_semaphore()
    def exists(step):
        return me >= -step if step < 0 else me < n - step

    def signal(step):
        @pl.when(exists(step))
        def _():
            pl.semaphore_signal(
                barrier, inc=1, device_id=device(step), device_id_type=pl.DeviceIdType.MESH
            )

    for step in STEPS:
        signal(step)
    loads = [
        pltpu.make_async_copy(src, dst, local_sem.at[i])
        for i, (src, dst) in enumerate(
            [
                (counts_hbm, counts), (coef_hbm, coef), (b_hbm, b_own), (cell_hbm, cell),
                (near_hbm, near), (far_hbm, far), (prolong_hbm, prolong),
            ]
        )
    ]
    for c in loads:
        c.start()

    def remote(src, dst, send, recv, slot):
        copy = pltpu.make_async_remote_copy(
            src_ref=src, dst_ref=dst, send_sem=send.at[slot], recv_sem=recv.at[slot],
            device_id=device(STEPS[slot]), device_id_type=pl.DeviceIdType.MESH,
        )
        return copy, STEPS[slot]

    def start(pair):
        @pl.when(exists(pair[1]))
        def _():
            pair[0].start()

    def received(pair):
        @pl.when(exists(-pair[1]))
        def _():
            pair[0].wait_recv()

    def sent(pair):
        @pl.when(exists(pair[1]))
        def _():
            pair[0].wait_send()

    loads[0].wait()
    loads[1].wait()
    def count(t):
        return jnp.minimum(jnp.maximum(counts[t], half), cap)

    live = count(me)
    c_live = lax.div(live, 8)
    for i in range(cap // 128):
        wide_a[pl.ds(depth + 128 * i, 128), :] = columns(coef[pl.ds(i, 1), :])
    mean = wide_a[pl.ds(depth, c_cap, stride=8), :]
    for c in range(1, 8):
        mean = mean + wide_a[pl.ds(depth + c, c_cap, stride=8), :]
    mean = mean * 0.125
    c_coef[pl.ds(0, c_cap), :] = jnp.zeros((c_cap, 128), F32)
    c_coef[pl.ds(c_cap, c_cap), :] = mean
    c_own[pl.ds(0, c_cap), :] = jnp.zeros((c_cap, 128), F32)
    both = jnp.concatenate([mean, c_coef[pl.ds(c_live, c_cap), :]], 0)
    meta[pl.ds(0, 4), :] = coef[...]
    meta[pl.ds(4, 4), :] = jnp.transpose(both)[0:4, :]

    loads[2].wait()
    tail[...] = b_own[pl.ds(8 * (c_live - depth // 8), depth), :]
    pl.semaphore_wait(barrier, jnp.minimum(me, 3) + jnp.minimum(n - 1 - me, 3))
    halo = [
        remote(tail, ghost_low, b_send, b_recv, 0),
        remote(b_own.at[pl.ds(0, depth)], ghost_high.at[pl.ds(half, depth)], b_send, b_recv, 1),
    ]
    metas = [
        remote(meta, meta_in.at[i], m_send, m_recv, i) for i in range(len(STEPS))
    ]
    for c in metas[:2] + halo + metas[2:]:
        start(c)

    for c in loads[3:6]:
        c.wait()
    near_m = near[...]
    far_m = far[...]
    cell_m = cell[...]
    blocks = [cell_m, -near_m, -jnp.transpose(near_m), -far_m, -jnp.transpose(far_m)]
    for i, m in enumerate(blocks):
        high, low = split(m)
        main_w[pl.ds(0, 128), pl.ds(128 * i, 128)] = high
        main_w[pl.ds(128, 128), pl.ds(128 * i, 128)] = high
        low_w[:, pl.ds(128 * i, 128)] = low
    eye = lax.broadcasted_iota(jnp.int32, (128, 128), 0) == lax.broadcasted_iota(
        jnp.int32, (128, 128), 1
    )
    diag = jnp.sum(jnp.where(eye, cell_m, 0.0), axis=0, keepdims=True)
    loads[6].wait()
    for i in range(8):
        m = prolong[i]
        high, low = split(m)
        pro_w[pl.ds(0, 128), pl.ds(128 * i, 128)] = high
        pro_w[pl.ds(128, 128), pl.ds(128 * i, 128)] = high
        pro_low[:, pl.ds(128 * i, 128)] = low
        high, low = split(jnp.transpose(m))
        rest_w[pl.ds(256 * i, 128), :] = high
        rest_w[pl.ds(256 * i + 128, 128), :] = high
        rest_low[pl.ds(128 * i, 128), :] = low
    y[:, pl.ds(0, stride), :] = jnp.zeros((5, stride, 128), F32)
    y[:, pl.ds(stride + total, stride), :] = jnp.zeros((5, stride, 128), F32)

    for c in metas[:2]:
        received(c)
    for i in range(cap // 128):
        a_left[pl.ds(128 * i, 128), :] = columns(meta_in[0, pl.ds(i, 1), :])
    for i in range(2):
        a_high[pl.ds(half + 128 * i, 128), :] = columns(meta_in[1, pl.ds(i, 1), :])
    has_prev = me > 0
    has_next = me < n - 1
    left_live = count(at(-1))
    low_limit = jnp.where(has_prev, 0, depth)
    high_limit = depth + live + jnp.where(has_next, depth, 0)
    shift = 8 * (cap // 8 - c_live)
    n1 = lax.div(left_live, 8)
    a_low = a_left[pl.ds(8 * (n1 - depth // 8), depth), :]
    own_a = wide_a[pl.ds(depth + half, half), :]
    more_a = a_high[pl.ds(shift, cap + depth - half), :]
    index = rows_of(depth + half, cap + depth - half)
    inside = index < depth + live
    wide_a[pl.ds(0, depth), :] = jnp.where(rows_of(0, depth) >= low_limit, a_low, 0.0)
    padded_a = jnp.concatenate([own_a, jnp.zeros((depth, 128), F32)], 0)
    wide_a[pl.ds(depth + half, cap + depth - half), :] = jnp.where(
        index < high_limit, jnp.where(inside, padded_a, more_a), 0.0
    )
    all_rows = rows_of(0, total)
    is_live = (all_rows >= low_limit) & (all_rows < high_limit)
    wide_j[...] = jnp.where(is_live, 1.0 / (jnp.where(is_live, wide_a[...], 16.0) + diag), 0.0)

    for c in halo:
        received(c)
    wide_b[pl.ds(0, depth), :] = jnp.where(
        rows_of(0, depth) >= low_limit, ghost_low[...], 0.0
    )
    wide_b[pl.ds(depth, half), :] = b_own[pl.ds(0, half), :]
    padded_b = jnp.concatenate(
        [b_own[pl.ds(half, half), :], jnp.zeros((depth, 128), F32)], 0
    )
    more_b = ghost_high[pl.ds(shift, cap + depth - half), :]
    wide_b[pl.ds(depth + half, cap + depth - half), :] = jnp.where(
        index < high_limit, jnp.where(inside, padded_b, more_b), 0.0
    )

    def products(field, low, high):
        first, size = low - stride, high - low + 2 * stride
        hi, lo = split(field[pl.ds(first, size), :])
        pair = jnp.concatenate([hi, lo], 1)
        for start in range(0, 640, 256):
            width = min(256, 640 - start)
            part = jnp.dot(
                pair, main_w[:, pl.ds(start, width)], preferred_element_type=F32
            ) + jnp.dot(hi, low_w[:, pl.ds(start, width)], preferred_element_type=F32)
            for k in range(width // 128):
                y[start // 128 + k, pl.ds(stride + first, size), :] = part[
                    :, 128 * k : 128 * k + 128
                ]

    def applied(field, coefs, low, high):
        size = high - low
        row = stride + low
        return (
            coefs[pl.ds(low, size), :] * field[pl.ds(low, size), :]
            + y[0, pl.ds(row, size), :]
            + y[1, pl.ds(row + 1, size), :]
            + y[2, pl.ds(row - 1, size), :]
            + y[3, pl.ds(row + stride, size), :]
            + y[4, pl.ds(row - stride, size), :]
        )

    def residual(field, coefs, source, low, high):
        products(field, low, high)
        return source[pl.ds(low, high - low), :] - applied(field, coefs, low, high)

    def improve(field, update, coefs, scale, source, low, high, keep, gain):
        rows = pl.ds(low, high - low)
        r = residual(field, coefs, source, low, high)
        step = gain * scale[rows, :] * r
        if keep is not None:
            step = keep * update[rows, :] + step
        update[rows, :] = step
        field[rows, :] = field[rows, :] + step

    pairs = weights_of()
    first = wide_j[...] * wide_b[...] * (1.0 / CENTER)
    x[...] = first
    d[...] = first
    low, high = stride, total - stride
    for keep, gain in pairs:
        improve(x, d, wide_a, wide_j, wide_b, low, high, keep, gain)
        low, high = low + stride, high - stride
    res[...] = residual(x, wide_a, wide_b, depth, depth + cap)

    acc = jnp.zeros((c_cap, 128), F32)
    for i in range(8):
        hi, lo = split(res[pl.ds(i, c_cap, stride=8), :])
        acc = acc + jnp.dot(
            jnp.concatenate([hi, lo], 1), rest_w[pl.ds(256 * i, 256), :],
            preferred_element_type=F32,
        )
        acc = acc + jnp.dot(hi, rest_low[pl.ds(128 * i, 128), :], preferred_element_type=F32)
    c_own[pl.ds(c_cap, c_cap), :] = acc
    c_tail[...] = c_own[pl.ds(c_live, c_cap), :]
    x_tail[...] = x[pl.ds(8 * c_live, depth), :]
    x_head[...] = x[pl.ds(depth, depth), :]
    halo_x = [
        remote(x_tail, x_low, x_send, x_recv, 0),
        remote(x_head, x_high.at[pl.ds(half, depth)], x_send, x_recv, 1),
    ]
    coarse = [
        remote(c_tail, l1.at[pl.ds(16, c_cap)], c_send, c_recv, 0),
        remote(c_own.at[pl.ds(c_cap, c_cap)], r1.at[pl.ds(32, c_cap)], c_send, c_recv, 1),
        remote(c_tail.at[pl.ds(c_cap - 48, 48)], l2.at[pl.ds(0, 48)], c_send, c_recv, 2),
        remote(c_own.at[pl.ds(c_cap, 48)], r2.at[pl.ds(64, 48)], c_send, c_recv, 3),
        remote(c_tail.at[pl.ds(c_cap - 16, 16)], l3.at[pl.ds(0, 16)], c_send, c_recv, 4),
        remote(c_own.at[pl.ds(c_cap, 16)], r3.at[pl.ds(96, 16)], c_send, c_recv, 5),
    ]
    for c in coarse + halo_x:
        start(c)
    for c in metas[2:]:
        received(c)
    for i, (ref, at_row, first, size) in enumerate(
        [
            (k1, 16, 128 - c_cap, c_cap), (q1, 32, 0, c_cap),
            (k2, 0, 128 - 48, 48), (q2, 64, 0, 48),
            (k3, 0, 128 - 16, 16), (q3, 96, 0, 16),
        ]
    ):
        ref[pl.ds(at_row, size), :] = columns(meta_in[i, pl.ds(4, 1), :])[first : first + size]


    n2 = lax.div(count(at(-2)), 8)
    p1 = lax.div(count(at(1)), 8)
    p2 = lax.div(count(at(2)), 8)
    e2 = base - n1
    e3 = e2 - n2
    s1 = base + c_live
    s2 = s1 + p1
    s3 = s2 + p2
    c_low = jnp.where(
        me >= 3, e3 - 16, jnp.where(me == 2, e3, jnp.where(me == 1, e2, base))
    )
    c_high = jnp.where(
        me + 3 < n, s3 + 16, jnp.where(me + 3 == n, s3, jnp.where(me + 2 == n, s2, s1))
    )

    def gathered(target, own, b1, b2, b3, a1, a2, a3):
        r = rows_of(0, base)
        v2 = jnp.concatenate([b2[pl.ds(48 - e2, 48), :], jnp.zeros((base - 48, 128), F32)], 0)
        v3 = jnp.concatenate([b3[pl.ds(16 - e3, 16), :], jnp.zeros((base - 16, 128), F32)], 0)
        value = jnp.where(r >= e2, b1[...], jnp.where(r >= e3, v2, v3))
        target[pl.ds(0, base), :] = jnp.where(r >= c_low, value, 0.0)
        r = rows_of(base, c_cap + base)
        v0 = jnp.concatenate([own, jnp.zeros((base, 128), F32)], 0)
        v1 = jnp.concatenate([jnp.zeros((32, 128), F32), a1[pl.ds(c_cap - c_live, 112), :]], 0)
        v2 = jnp.concatenate([jnp.zeros((64, 128), F32), a2[pl.ds(208 - s2, 80), :]], 0)
        v3 = jnp.concatenate([jnp.zeros((96, 128), F32), a3[pl.ds(272 - s3, 48), :]], 0)
        value = jnp.where(
            r < s1, v0, jnp.where(r < s2, v1, jnp.where(r < s3, v2, v3))
        )
        target[pl.ds(base, c_cap + base), :] = jnp.where(r < c_high, value, 0.0)

    gathered(c_a, mean, k1, k2, k3, q1, q2, q3)
    r = rows_of(0, c_total)
    c_live_rows = (r >= c_low) & (r < c_high)
    c_j[...] = jnp.where(
        c_live_rows, 1.0 / (jnp.where(c_live_rows, c_a[...], 16.0) + diag), 0.0
    )
    for c in coarse:
        received(c)
    gathered(c_b, acc, l1, l2, l3, r1, r2, r3)
    first = c_j[...] * c_b[...] * (1.0 / CENTER)
    c_x[...] = first
    c_d[...] = first
    for i, (keep, gain) in enumerate(pairs):
        low = stride * (i + 1)
        improve(c_x, c_d, c_a, c_j, c_b, low, c_total - low, keep, gain)

    for c in halo_x:
        received(c)
    x[pl.ds(0, depth), :] = jnp.where(rows_of(0, depth) >= low_limit, x_low[...], 0.0)
    more_x = x_high[pl.ds(shift, cap + depth - half), :]
    x[pl.ds(depth + half, cap + depth - half), :] = jnp.where(
        inside,
        x[pl.ds(depth + half, cap + depth - half), :],
        jnp.where(index < high_limit, more_x, 0.0),
    )
    edge = depth // 8
    rows = c_cap + 2 * edge
    hi, lo = split(c_x[pl.ds(base - edge, rows), :])
    pair = jnp.concatenate([hi, lo], 1)
    for start in range(0, 1024, 256):
        part = jnp.dot(
            pair, pro_w[:, pl.ds(start, 256)], preferred_element_type=F32
        ) + jnp.dot(hi, pro_low[:, pl.ds(start, 256)], preferred_element_type=F32)
        for k in range(2):
            where = pl.ds(start // 128 + k, rows, stride=8)
            x[where, :] = x[where, :] + part[:, 128 * k : 128 * k + 128]

    low, high = stride, total - stride
    improve(x, d, wide_a, wide_j, wide_b, low, high, None, 1.0 / CENTER)
    for keep, gain in pairs:
        low, high = low + stride, high - stride
        improve(x, d, wide_a, wide_j, wide_b, low, high, keep, gain)
    out_ref[...] = jnp.where(rows_of(0, cap) < live, x[pl.ds(depth, cap), :], 0.0)
    for c in halo + metas + coarse + halo_x:
        sent(c)


def shards(n, lanes, right_side, cell_coef, fine_count, cell_matrix, face_near, face_far, prolong):
    cap = right_side.shape[0]
    stride = cap // 16
    depth = 3 * stride
    total = cap + 2 * depth
    c_cap = cap // 8
    base = c_cap + 16
    c_total = 2 * base + c_cap
    half = cap // 2

    def vmem(*shape, dtype=F32):
        return pltpu.VMEM(shape, dtype)

    scratch = [
        pltpu.SMEM(fine_count.shape, jnp.int32), vmem(cap, 128), vmem(4, 128),
        vmem(128, 128), vmem(128, 128), vmem(128, 128), vmem(8, 128, 128),
        vmem(depth, 128), vmem(depth, 128), vmem(cap + depth, 128), vmem(8, 128),
        vmem(6, 8, 128),
        vmem(cap, 128), vmem(cap + depth, 128), vmem(total, 128), vmem(total, 128),
        vmem(total, 128), vmem(total, 128), vmem(total, 128),
        vmem(5, total + 2 * stride, 128), vmem(cap, 128),
        vmem(256, 640, dtype=BF16), vmem(128, 640, dtype=BF16),
        vmem(2048, 128, dtype=BF16), vmem(1024, 128, dtype=BF16),
        vmem(256, 1024, dtype=BF16), vmem(128, 1024, dtype=BF16),
        vmem(2 * c_cap, 128), vmem(c_cap, 128), vmem(2 * c_cap, 128),
    ]
    for _ in range(2):
        scratch += [vmem(base, 128)] * 3 + [vmem(base + c_cap, 128)] * 3
    scratch += [vmem(c_total, 128)] * 5
    scratch += [vmem(depth, 128), vmem(depth, 128), vmem(depth, 128), vmem(cap + depth, 128)]
    dma = pltpu.SemaphoreType.DMA
    scratch += [dma((7,)), dma((2,)), dma((2,)), dma((6,)), dma((6,)), dma((6,)), dma((6,)), dma((2,)), dma((2,))]
    return pl.pallas_call(
        functools.partial(cycle, n, lanes, cap),
        out_shape=jax.ShapeDtypeStruct(right_side.shape, F32),
        in_specs=[pl.BlockSpec(memory_space=pltpu.MemorySpace.HBM)] * 7,
        out_specs=pl.BlockSpec(memory_space=pltpu.VMEM),
        scratch_shapes=scratch,
        compiler_params=pltpu.CompilerParams(
            collective_id=0, has_side_effects=True, vmem_limit_bytes=32 * 2**20
        ),
        name="cycle",
    )(
        *(
            pltpu.with_memory_space_constraint(v, pltpu.MemorySpace.HBM)
            for v in (
                fine_count, right_side, cell_coef.reshape(4, 128), cell_matrix, face_near,
                face_far, prolong,
            )
        )
    )


def solution(mesh):
    placed = (P(("sfc", "lvl"), None), P(("sfc", "lvl")), P(), P(), P(), P(), P())
    lanes = mesh.shape["lvl"]
    n = mesh.shape["sfc"] * lanes
    return jax.shard_map(
        functools.partial(shards, n, lanes),
        mesh=mesh, in_specs=placed, out_specs=P(("sfc", "lvl"), None), check_vma=False,
    )
```

```python
import functools

import jax
import jax.numpy as jnp
from jax import lax
from jax.experimental import pallas as pl
from jax.experimental.pallas import tpu as pltpu
from jax.sharding import PartitionSpec as P

DEG = 3
CENTER = 1.025
RADIUS = 0.775
STEPS = (1, -1, 2, -2, 3, -3)
F32 = jnp.float32
BF16 = jnp.bfloat16


def weights_of():
    ratio = CENTER / RADIUS
    prev = 1.0 / ratio
    pairs = []
    for _ in range(DEG - 1):
        new = 1.0 / (2.0 * ratio - prev)
        pairs.append((new * prev, 2.0 * new / RADIUS))
        prev = new
    return pairs


def split(x):
    high = x.astype(BF16)
    low = (x - high.astype(F32)).astype(BF16)
    return high, low


def rows_of(start, size):
    return start + lax.broadcasted_iota(jnp.int32, (size, 128), 0)


def columns(row):
    return jnp.transpose(jnp.broadcast_to(row, (128, 128)))


def cycle(
    n, lanes, cap,
    counts_hbm, b_hbm, coef_hbm, cell_hbm, near_hbm, far_hbm, prolong_hbm,
    out_ref,
    counts, b_own, coef, cell, near, far, prolong,
    tail, ghost_low, ghost_high, meta, meta_in,
    a_left, a_high, wide_b, wide_a, wide_j, x, d, y, res,
    strip1, strip2, strip3, strip_d,
    main_w, mix_w, rest_w, pro_w, pro_low,
    c_own, c_tail, c_coef, l1, l2, r1, r2, r3, k1, k2, k3, q1, q2, q3,
    c_b, c_a, c_j, c_x, c_d, x_head, x_high,
    local_sem, b_send, b_recv, m_send, m_recv, c_send, c_recv, x_send, x_recv,
):
    stride = cap // 16
    left = 6 * stride
    right = 3 * stride
    total = left + cap + right
    inner = left + cap
    c_cap = cap // 8
    edge = right // 8
    base = c_cap + 16
    c_total = base + c_cap + base
    half = cap // 2
    more = half + right
    me = lax.axis_index("sfc") * lanes + lax.axis_index("lvl")

    def at(step):
        return lax.rem(me + (step + n), n)

    def device(step):
        t = at(step)
        return (lax.div(t, lanes), lax.rem(t, lanes))

    def exists(step):
        return me >= -step if step < 0 else me < n - step

    barrier = pltpu.get_barrier_semaphore()

    def signal(step):
        @pl.when(exists(step))
        def _():
            pl.semaphore_signal(
                barrier, inc=1, device_id=device(step), device_id_type=pl.DeviceIdType.MESH
            )

    for step in STEPS:
        signal(step)
    loads = [
        pltpu.make_async_copy(src, dst, local_sem.at[i])
        for i, (src, dst) in enumerate(
            [
                (counts_hbm, counts), (coef_hbm, coef), (b_hbm, b_own), (cell_hbm, cell),
                (near_hbm, near), (far_hbm, far), (prolong_hbm, prolong),
            ]
        )
    ]
    for c in loads:
        c.start()

    def remote(src, dst, send, recv, slot, sem=None):
        sem = slot if sem is None else sem
        copy = pltpu.make_async_remote_copy(
            src_ref=src, dst_ref=dst, send_sem=send.at[sem], recv_sem=recv.at[sem],
            device_id=device(STEPS[slot]), device_id_type=pl.DeviceIdType.MESH,
        )
        return copy, STEPS[slot]

    def start(pair):
        @pl.when(exists(pair[1]))
        def _():
            pair[0].start()

    def received(pair):
        @pl.when(exists(-pair[1]))
        def _():
            pair[0].wait_recv()

    def sent(pair):
        @pl.when(exists(pair[1]))
        def _():
            pair[0].wait_send()

    loads[0].wait()
    loads[1].wait()

    def count(t):
        return jnp.minimum(jnp.maximum(counts[t], half), cap)

    live = count(me)
    c_live = lax.div(live, 8)
    for i in range(cap // 128):
        wide_a[pl.ds(left + 128 * i, 128), :] = columns(coef[pl.ds(i, 1), :])
    mean = wide_a[pl.ds(left, c_cap, stride=8), :]
    for c in range(1, 8):
        mean = mean + wide_a[pl.ds(left + c, c_cap, stride=8), :]
    mean = mean * 0.125
    c_coef[pl.ds(0, c_cap), :] = jnp.zeros((c_cap, 128), F32)
    c_coef[pl.ds(c_cap, c_cap), :] = mean
    both = jnp.concatenate([mean, c_coef[pl.ds(c_live, c_cap), :]], 0)
    meta[pl.ds(0, 4), :] = coef[...]
    meta[pl.ds(4, 4), :] = jnp.transpose(both)[0:4, :]

    loads[2].wait()
    tail[...] = b_own[pl.ds(8 * (c_live - left // 8), left), :]
    pl.semaphore_wait(barrier, jnp.minimum(me, 3) + jnp.minimum(n - 1 - me, 3))
    halo = [
        remote(tail, ghost_low, b_send, b_recv, 0),
        remote(b_own.at[pl.ds(0, right)], ghost_high.at[pl.ds(half, right)], b_send, b_recv, 1),
    ]
    metas = [
        remote(meta, meta_in.at[i], m_send, m_recv, i) for i in range(len(STEPS))
    ]
    for c in [metas[0], halo[0], metas[1], halo[1]] + metas[2:]:
        start(c)

    for c in loads[3:6]:
        c.wait()
    cell_m = cell[...]
    parts = [cell_m, -near[...], -jnp.transpose(near[...]), -far[...], -jnp.transpose(far[...])]
    parts = [split(m) for m in parts]
    (c_hi, c_lo), (n_hi, n_lo), (nt_hi, nt_lo), (f_hi, f_lo), (ft_hi, ft_lo) = parts
    for i, (upper, lower) in enumerate(
        [
            (n_hi, n_hi), (ft_hi, ft_hi), (nt_hi, nt_hi), (f_hi, f_hi), (c_hi, c_hi),
            (c_lo, jnp.zeros_like(c_lo)),
        ]
    ):
        main_w[pl.ds(0, 128), pl.ds(128 * i, 128)] = upper
        main_w[pl.ds(128, 128), pl.ds(128 * i, 128)] = lower
    for i, (upper, lower) in enumerate([(n_lo, f_lo), (ft_lo, nt_lo)]):
        mix_w[pl.ds(0, 128), pl.ds(128 * i, 128)] = upper
        mix_w[pl.ds(128, 128), pl.ds(128 * i, 128)] = lower
    eye = lax.broadcasted_iota(jnp.int32, (128, 128), 0) == lax.broadcasted_iota(
        jnp.int32, (128, 128), 1
    )
    diag = jnp.sum(jnp.where(eye, cell_m, 0.0), axis=0, keepdims=True)
    y[:, pl.ds(0, stride), :] = jnp.zeros((5, stride, 128), F32)
    y[:, pl.ds(stride + total, stride), :] = jnp.zeros((5, stride, 128), F32)
    for ref in (strip1, strip2, strip3):
        ref[pl.ds(8 * stride, stride), :] = jnp.zeros((stride, 128), F32)
    c_x[pl.ds(c_total, stride), :] = jnp.zeros((stride, 128), F32)
    x[pl.ds(inner, right + stride), :] = jnp.zeros((right + stride, 128), F32)
    wide_a[pl.ds(inner, right), :] = jnp.zeros((right, 128), F32)
    c_own[...] = jnp.zeros_like(c_own)
    res[pl.ds(right + cap, stride), :] = jnp.zeros((stride, 128), F32)

    def products(field, first, size):
        hi, lo = split(field[pl.ds(first, size), :])
        pair = jnp.concatenate([hi, lo], 1)
        ahead = field[pl.ds(first + stride - 1, size), :].astype(BF16)
        rows = pl.ds(stride + first, size)
        part = jnp.dot(
            pair, main_w[:, pl.ds(0, 256)], preferred_element_type=F32
        ) + jnp.dot(
            jnp.concatenate([hi, ahead], 1), mix_w[...], preferred_element_type=F32
        )
        y[1, rows, :] = part[:, :128]
        y[4, rows, :] = part[:, 128:]
        part = jnp.dot(pair, main_w[:, pl.ds(256, 256)], preferred_element_type=F32)
        y[2, rows, :] = part[:, :128]
        y[3, rows, :] = part[:, 128:]
        part = jnp.dot(pair, main_w[:, pl.ds(512, 256)], preferred_element_type=F32)
        y[0, rows, :] = part[:, :128] + part[:, 128:]

    def residual(field, coefs, source, low, high, shift=0):
        size = high - low
        products(field, low - stride, size + 2 * stride)
        row = stride + low
        wide = pl.ds(low + shift, size)
        return source[wide, :] - (
            coefs[wide, :] * field[pl.ds(low, size), :]
            + y[0, pl.ds(row, size), :]
            + y[1, pl.ds(row + 1, size), :]
            + y[2, pl.ds(row - 1, size), :]
            + y[3, pl.ds(row + stride, size), :]
            + y[4, pl.ds(row - stride, size), :]
        )

    def improve(field, update, coefs, scale, source, low, high, keep, gain):
        rows = pl.ds(low, high - low)
        step = gain * scale[rows, :] * residual(field, coefs, source, low, high)
        if keep is not None:
            step = keep * update[rows, :] + step
        update[rows, :] = step
        field[rows, :] = field[rows, :] + step

    pairs = weights_of()
    has_prev = me > 0
    has_next = me < n - 1

    own = pl.ds(left, cap)
    own_rows = rows_of(0, cap) < live
    own_j = jnp.where(own_rows, 1.0 / (wide_a[own, :] + diag), 0.0)
    own_b = jnp.where(own_rows, b_own[...], 0.0)
    wide_j[own, :] = own_j
    wide_b[own, :] = own_b
    wide_j[pl.ds(inner, right), :] = jnp.zeros((right, 128), F32)
    wide_b[pl.ds(inner, right), :] = jnp.zeros((right, 128), F32)
    first = own_j * own_b * (1.0 / CENTER)
    x[own, :] = first
    d[own, :] = first
    strip1[pl.ds(left, 2 * stride), :] = first[: 2 * stride]
    improve(x, d, wide_a, wide_j, wide_b, left + stride, inner, *pairs[0])
    strip2[pl.ds(left, 2 * stride), :] = x[pl.ds(left + stride, 2 * stride), :]
    strip_d[pl.ds(left, 2 * stride), :] = d[pl.ds(left + stride, 2 * stride), :]
    improve(x, d, wide_a, wide_j, wide_b, left + 2 * stride, inner, *pairs[1])
    strip3[pl.ds(left, 2 * stride), :] = x[pl.ds(left + 2 * stride, 2 * stride), :]
    res[pl.ds(2 * right, cap - right), :] = residual(
        x, wide_a, wide_b, left + right, inner
    )

    loads[6].wait()
    for i in range(8):
        m = prolong[i]
        high, low = split(m)
        pro_w[pl.ds(0, 128), pl.ds(128 * i, 128)] = high
        pro_w[pl.ds(128, 128), pl.ds(128 * i, 128)] = high
        pro_low[:, pl.ds(128 * i, 128)] = low
        high, low = split(jnp.transpose(m))
        for k in range(2):
            rest_w[pl.ds(256 * i + 128 * k, 128), pl.ds(0, 128)] = high
            rest_w[pl.ds(256 * i + 128 * k, 128), pl.ds(128, 128)] = low

    low_limit = jnp.where(has_prev, 0, left)
    left_rows = rows_of(0, left) >= low_limit
    received(metas[0])
    for i in range(cap // 128):
        a_left[pl.ds(128 * i, 128), :] = columns(meta_in[0, pl.ds(i, 1), :])
    n1 = lax.div(count(at(-1)), 8)
    a_low = jnp.where(left_rows, a_left[pl.ds(8 * (n1 - left // 8), left), :], 0.0)
    wide_a[pl.ds(0, left), :] = a_low
    j_low = jnp.where(left_rows, 1.0 / (jnp.where(left_rows, a_low, 16.0) + diag), 0.0)
    wide_j[pl.ds(0, left), :] = j_low

    received(halo[0])
    b_low = jnp.where(left_rows, ghost_low[...], 0.0)
    wide_b[pl.ds(0, left), :] = b_low
    strip1[pl.ds(0, left), :] = j_low * b_low * (1.0 / CENTER)
    low, high = stride, 7 * stride
    middle = pl.ds(low, high - low)
    keep, gain = pairs[0]
    step = gain * wide_j[middle, :] * residual(strip1, wide_a, wide_b, low, high)
    step = keep * strip1[middle, :] + step
    strip_d[pl.ds(0, left), :] = step
    strip2[pl.ds(0, left), :] = strip1[middle, :] + step
    keep, gain = pairs[1]
    step = gain * wide_j[pl.ds(low + stride, left), :] * residual(
        strip2, wide_a, wide_b, low, high, stride
    )
    step = keep * strip_d[middle, :] + step
    strip3[pl.ds(0, left), :] = strip2[middle, :] + step
    res[pl.ds(0, left), :] = residual(strip3, wide_a, wide_b, low, high, 2 * stride)

    acc = jnp.zeros((base, 256), F32)
    for i in range(8):
        hi, lo = split(res[pl.ds(i, base, stride=8), :])
        acc = acc + jnp.dot(
            jnp.concatenate([hi, lo], 1), rest_w[pl.ds(256 * i, 256), :],
            preferred_element_type=F32,
        )
    front = c_cap + 8
    c_own[pl.ds(front, base), :] = acc[:, :128] + acc[:, 128:]
    c_tail[...] = c_own[pl.ds(8 + c_live, c_cap), :]
    coarse = [
        remote(c_tail, l1.at[pl.ds(8, c_cap)], c_send, c_recv, 0),
        remote(c_own.at[pl.ds(front, base)], r1.at[pl.ds(40, base)], c_send, c_recv, 1),
        remote(c_tail.at[pl.ds(c_cap - 32, 32)], l2.at[pl.ds(8, 32)], c_send, c_recv, 2),
        remote(c_own.at[pl.ds(front, 56)], r2.at[pl.ds(72, 56)], c_send, c_recv, 3),
        remote(c_own.at[pl.ds(front, 24)], r3.at[pl.ds(104, 24)], c_send, c_recv, 5, 4),
    ]
    for c in coarse:
        start(c)
    x[pl.ds(2 * stride, left), :] = strip3[pl.ds(0, left), :]
    x_head[...] = x[pl.ds(left - 2 * stride, 5 * stride), :]
    halo_x = remote(x_head, x_high.at[pl.ds(half, 5 * stride)], x_send, x_recv, 1, 0)
    start(halo_x)

    for c in metas[1:]:
        received(c)
    for i in range(2):
        a_high[pl.ds(half + 128 * i, 128), :] = columns(meta_in[1, pl.ds(i, 1), :])
    for i, (ref, at_row, top, size) in enumerate(
        [
            (k1, 16, 128 - c_cap, c_cap), (q1, 32, 0, c_cap),
            (k2, 0, 128 - 48, 48), (q2, 64, 0, 48),
            (k3, 0, 128 - 16, 16), (q3, 96, 0, 16),
        ]
    ):
        ref[pl.ds(at_row, size), :] = columns(meta_in[i, pl.ds(4, 1), :])[top : top + size]
    received(halo[1])
    shift = 8 * (cap // 8 - c_live)
    index = rows_of(half, more)
    limit = live + jnp.where(has_next, right, 0)
    late = pl.ds(left + half, more)
    old = index < live
    new = index < limit
    late_a = jnp.where(
        new, jnp.where(old, wide_a[late, :], a_high[pl.ds(shift, more), :]), 0.0
    )
    wide_a[late, :] = late_a
    wide_j[late, :] = jnp.where(new, 1.0 / (jnp.where(new, late_a, 16.0) + diag), 0.0)
    wide_b[late, :] = jnp.where(
        new, jnp.where(old, wide_b[late, :], ghost_high[pl.ds(shift, more), :]), 0.0
    )

    n2 = lax.div(count(at(-2)), 8)
    p1 = lax.div(count(at(1)), 8)
    p2 = lax.div(count(at(2)), 8)
    e2 = base - n1
    e3 = e2 - n2
    s1 = base + c_live
    s2 = s1 + p1
    s3 = s2 + p2
    reach = c_cap + edge
    c_low = jnp.maximum(
        base - reach, jnp.where(me >= 3, 0, jnp.where(me == 2, e3, jnp.where(me == 1, e2, base)))
    )
    c_high = jnp.minimum(
        s1 + reach,
        jnp.where(
            me + 3 < n, s3 + reach,
            jnp.where(me + 3 == n, s3, jnp.where(me + 2 == n, s2, s1)),
        ),
    )

    def zeros(rows):
        return jnp.zeros((rows, 128), F32)

    r = rows_of(0, base)
    v2 = jnp.concatenate([k2[pl.ds(48 - e2, 48), :], zeros(base - 48)], 0)
    v3 = jnp.concatenate([k3[pl.ds(16 - e3, 16), :], zeros(base - 16)], 0)
    value = jnp.where(r >= e2, k1[...], jnp.where(r >= e3, v2, v3))
    c_a[pl.ds(0, base), :] = jnp.where(r >= c_low, value, 0.0)
    r = rows_of(base, c_cap + base)
    v0 = jnp.concatenate([mean, zeros(base)], 0)
    v1 = jnp.concatenate([zeros(32), q1[pl.ds(c_cap - c_live, 112), :]], 0)
    v2 = jnp.concatenate([zeros(64), q2[pl.ds(208 - s2, 80), :]], 0)
    v3 = jnp.concatenate([zeros(96), q3[pl.ds(272 - s3, 48), :]], 0)
    value = jnp.where(r < s1, v0, jnp.where(r < s2, v1, jnp.where(r < s3, v2, v3)))
    c_a[pl.ds(base, c_cap + base), :] = jnp.where(r < c_high, value, 0.0)
    r = rows_of(0, c_total)
    c_live_rows = (r >= c_low) & (r < c_high)
    c_j[...] = jnp.where(
        c_live_rows, 1.0 / (jnp.where(c_live_rows, c_a[...], 16.0) + diag), 0.0
    )

    for c in coarse:
        received(c)
    o1 = s1 - edge
    o2 = s2 - edge
    o3 = s3 - edge
    t1 = jnp.where(me == n - 1, c_total, o1)
    t2 = jnp.where(me == n - 2, c_total, o2)
    t3 = jnp.where(me == n - 3, c_total, o3)
    f2 = e2 - edge
    r = rows_of(0, front)
    v1 = l1[pl.ds(4, front), :]
    v2 = jnp.concatenate([l2[pl.ds(40 - f2, 40), :], zeros(front - 40)], 0)
    value = jnp.where(
        r >= base - edge, c_own[pl.ds(4, front), :], jnp.where(r >= f2, v1, v2)
    )
    c_b[pl.ds(0, front), :] = jnp.where(r >= c_low, value, 0.0)
    r = rows_of(front, c_total - front)
    v0 = jnp.concatenate([c_own[pl.ds(front + 4, base), :], zeros(front)], 0)
    v1 = jnp.concatenate([zeros(24), r1[pl.ds(136 - o1, 128), :]], 0)
    v2 = jnp.concatenate([zeros(56), r2[pl.ds(200 - o2, 96), :]], 0)
    v3 = jnp.concatenate([zeros(88), r3[pl.ds(264 - o3, 64), :]], 0)
    value = jnp.where(r < t1, v0, jnp.where(r < t2, v1, jnp.where(r < t3, v2, v3)))
    c_b[pl.ds(front, c_total - front), :] = jnp.where(
        (r >= c_low) & (r < c_high), value, 0.0
    )
    first = c_j[...] * c_b[...] * (1.0 / CENTER)
    c_x[pl.ds(0, c_total), :] = first
    c_d[...] = first
    for i, (keep, gain) in enumerate(pairs):
        low = stride * (i + 1)
        improve(c_x, c_d, c_a, c_j, c_b, low, c_total - low, keep, gain)

    received(halo_x)
    index = rows_of(left, cap + right - left)
    keep_x = live - jnp.where(has_next, 2 * stride, 0)
    late = pl.ds(2 * left, cap + right - left)
    x[late, :] = jnp.where(
        index < limit,
        jnp.where(index < keep_x, x[late, :], x_high[pl.ds(shift, cap + right - left), :]),
        0.0,
    )
    rows = c_cap + 2 * edge
    hi, lo = split(c_x[pl.ds(base - edge, rows), :])
    pair = jnp.concatenate([hi, lo], 1)
    for begin in range(0, 1024, 256):
        part = jnp.dot(
            pair, pro_w[:, pl.ds(begin, 256)], preferred_element_type=F32
        ) + jnp.dot(hi, pro_low[:, pl.ds(begin, 256)], preferred_element_type=F32)
        for k in range(2):
            where = pl.ds(right + begin // 128 + k, rows, stride=8)
            x[where, :] = x[where, :] + part[:, 128 * k : 128 * k + 128]

    low, high = left - 2 * stride, total - stride
    improve(x, d, wide_a, wide_j, wide_b, low, high, None, 1.0 / CENTER)
    for keep, gain in pairs:
        low, high = low + stride, high - stride
        improve(x, d, wide_a, wide_j, wide_b, low, high, keep, gain)
    out_ref[...] = jnp.where(own_rows, x[own, :], 0.0)
    for c in halo + metas + coarse + [halo_x]:
        sent(c)


def shards(n, lanes, right_side, cell_coef, fine_count, cell_matrix, face_near, face_far, prolong):
    cap = right_side.shape[0]
    stride = cap // 16
    left = 6 * stride
    right = 3 * stride
    total = left + cap + right
    c_cap = cap // 8
    base = c_cap + 16
    c_total = 2 * base + c_cap
    half = cap // 2

    def vmem(*shape, dtype=F32):
        return pltpu.VMEM(shape, dtype)

    scratch = [
        pltpu.SMEM(fine_count.shape, jnp.int32), vmem(cap, 128), vmem(4, 128),
        vmem(128, 128), vmem(128, 128), vmem(128, 128), vmem(8, 128, 128),
        vmem(left, 128), vmem(left, 128), vmem(cap + right, 128), vmem(8, 128),
        vmem(6, 8, 128),
        vmem(cap, 128), vmem(cap + right, 128), vmem(total, 128), vmem(total, 128),
        vmem(total, 128), vmem(total + stride, 128), vmem(total, 128),
        vmem(5, total + 2 * stride, 128), vmem(cap + right + stride, 128),
        vmem(9 * stride, 128), vmem(9 * stride, 128), vmem(9 * stride, 128),
        vmem(8 * stride, 128),
        vmem(256, 768, dtype=BF16), vmem(256, 256, dtype=BF16),
        vmem(2048, 256, dtype=BF16),
        vmem(256, 1024, dtype=BF16), vmem(128, 1024, dtype=BF16),
        vmem(160, 128), vmem(c_cap, 128), vmem(2 * c_cap, 128),
        vmem(88, 128), vmem(80, 128), vmem(168, 128), vmem(168, 128), vmem(168, 128),
    ]
    scratch += [vmem(base, 128)] * 3 + [vmem(base + c_cap, 128)] * 3
    scratch += [vmem(c_total, 128)] * 3 + [vmem(c_total + stride, 128), vmem(c_total, 128)]
    scratch += [vmem(5 * stride, 128), vmem(half + 416, 128)]
    dma = pltpu.SemaphoreType.DMA
    scratch += [dma((7,)), dma((2,)), dma((2,)), dma((6,)), dma((6,)), dma((5,)), dma((5,))]
    scratch += [dma((1,)), dma((1,))]
    return pl.pallas_call(
        functools.partial(cycle, n, lanes, cap),
        out_shape=jax.ShapeDtypeStruct(right_side.shape, F32),
        in_specs=[pl.BlockSpec(memory_space=pltpu.MemorySpace.HBM)] * 7,
        out_specs=pl.BlockSpec(memory_space=pltpu.VMEM),
        scratch_shapes=scratch,
        compiler_params=pltpu.CompilerParams(
            collective_id=0, has_side_effects=True, vmem_limit_bytes=32 * 2**20
        ),
        name="cycle",
    )(
        *(
            pltpu.with_memory_space_constraint(v, pltpu.MemorySpace.HBM)
            for v in (
                fine_count, right_side, cell_coef.reshape(4, 128), cell_matrix, face_near,
                face_far, prolong,
            )
        )
    )


def solution(mesh):
    placed = (P(("sfc", "lvl"), None), P(("sfc", "lvl")), P(), P(), P(), P(), P())
    lanes = mesh.shape["lvl"]
    n = mesh.shape["sfc"] * lanes
    return jax.shard_map(
        functools.partial(shards, n, lanes),
        mesh=mesh, in_specs=placed, out_specs=P(("sfc", "lvl"), None), check_vma=False,
    )
```

```python
import functools

import jax
import jax.numpy as jnp
from jax import lax
from jax.experimental import pallas as pl
from jax.experimental.pallas import tpu as pltpu
from jax.sharding import PartitionSpec as P

DEG = 3
CENTER = 1.025
RADIUS = 0.775
STEPS = (1, -1, 2, -2, 3, -3)
F32 = jnp.float32
BF16 = jnp.bfloat16


def weights_of():
    ratio = CENTER / RADIUS
    prev = 1.0 / ratio
    pairs = []
    for _ in range(DEG - 1):
        new = 1.0 / (2.0 * ratio - prev)
        pairs.append((new * prev, 2.0 * new / RADIUS))
        prev = new
    return pairs


def split(x):
    high = x.astype(BF16)
    low = (x - high.astype(F32)).astype(BF16)
    return high, low


def rows_of(start, size):
    return start + lax.broadcasted_iota(jnp.int32, (size, 128), 0)


def columns(row):
    return jnp.transpose(jnp.broadcast_to(row, (128, 128)))


def cycle(
    n, lanes, cap,
    counts_hbm, b_hbm, coef_hbm, cell_hbm, near_hbm, far_hbm, prolong_hbm,
    out_ref,
    counts, b_own, coef, cell, near, far, prolong,
    tail, ghost_low, ghost_high, meta, meta_in,
    a_left, a_high, wide_b, wide_a, wide_j, x, d, y, res,
    strip1, strip2, strip3, strip_d,
    main_w, mix_w, rest_w, pro_w, pro_low,
    c_own, c_tail, c_coef, l1, l2, r1, r2, r3, k1, k2, k3, q1, q2, q3,
    c_b, c_a, c_j, c_x, c_d, x_head, x_high,
    local_sem, b_send, b_recv, m_send, m_recv, c_send, c_recv, x_send, x_recv,
):
    stride = cap // 16
    left = 6 * stride
    right = 3 * stride
    total = left + cap + right
    inner = left + cap
    c_cap = cap // 8
    edge = right // 8
    base = c_cap + 16
    c_total = base + c_cap + base
    half = cap // 2
    more = half + right
    me = lax.axis_index("sfc") * lanes + lax.axis_index("lvl")

    def at(step):
        return lax.rem(me + (step + n), n)

    def device(step):
        t = at(step)
        return (lax.div(t, lanes), lax.rem(t, lanes))

    def exists(step):
        return me >= -step if step < 0 else me < n - step

    barrier = pltpu.get_barrier_semaphore()

    def signal(step):
        @pl.when(exists(step))
        def _():
            pl.semaphore_signal(
                barrier, inc=1, device_id=device(step), device_id_type=pl.DeviceIdType.MESH
            )

    for step in (-1, -2, -3):
        signal(step)
    loads = [
        pltpu.make_async_copy(src, dst, local_sem.at[i])
        for i, (src, dst) in enumerate(
            [
                (counts_hbm, counts), (coef_hbm, coef), (b_hbm, b_own), (cell_hbm, cell),
                (near_hbm, near), (far_hbm, far), (prolong_hbm, prolong),
            ]
        )
    ]
    for c in loads:
        c.start()

    def remote(src, dst, send, recv, slot, sem=None):
        sem = slot if sem is None else sem
        copy = pltpu.make_async_remote_copy(
            src_ref=src, dst_ref=dst, send_sem=send.at[sem], recv_sem=recv.at[sem],
            device_id=device(STEPS[slot]), device_id_type=pl.DeviceIdType.MESH,
        )
        return copy, STEPS[slot]

    def start(pair):
        @pl.when(exists(pair[1]))
        def _():
            pair[0].start()

    def received(pair):
        @pl.when(exists(-pair[1]))
        def _():
            pair[0].wait_recv()

    def sent(pair):
        @pl.when(exists(pair[1]))
        def _():
            pair[0].wait_send()

    loads[0].wait()
    loads[1].wait()

    def count(t):
        return jnp.minimum(jnp.maximum(counts[t], half), cap)

    live = count(me)
    c_live = lax.div(live, 8)
    for i in range(cap // 128):
        wide_a[pl.ds(left + 128 * i, 128), :] = columns(coef[pl.ds(i, 1), :])
    mean = wide_a[pl.ds(left, c_cap, stride=8), :]
    for c in range(1, 8):
        mean = mean + wide_a[pl.ds(left + c, c_cap, stride=8), :]
    mean = mean * 0.125
    c_coef[pl.ds(0, c_cap), :] = jnp.zeros((c_cap, 128), F32)
    c_coef[pl.ds(c_cap, c_cap), :] = mean
    both = jnp.concatenate([mean, c_coef[pl.ds(c_live, c_cap), :]], 0)
    meta[pl.ds(0, 4), :] = coef[...]
    meta[pl.ds(4, 4), :] = jnp.transpose(both)[0:4, :]

    loads[2].wait()
    tail[...] = b_own[pl.ds(8 * (c_live - left // 8), left), :]

    @pl.when(me < n - 1)
    def _():
        pl.semaphore_wait(barrier, jnp.minimum(n - 1 - me, 3))

    halo = [
        remote(tail, ghost_low, b_send, b_recv, 0),
        remote(b_own.at[pl.ds(0, right)], ghost_high.at[pl.ds(half, right)], b_send, b_recv, 1),
    ]
    metas = [
        remote(meta, meta_in.at[i], m_send, m_recv, i) for i in range(len(STEPS))
    ]
    early = lax.rem(lax.axis_index("sfc"), 2) == 1
    start(metas[0])

    @pl.when(early)
    def _():
        start(halo[0])

    start(metas[2])
    start(metas[4])

    for c in loads[3:6]:
        c.wait()
    cell_m = cell[...]
    parts = [cell_m, -near[...], -jnp.transpose(near[...]), -far[...], -jnp.transpose(far[...])]
    parts = [split(m) for m in parts]
    (c_hi, c_lo), (n_hi, n_lo), (nt_hi, nt_lo), (f_hi, f_lo), (ft_hi, ft_lo) = parts
    for i, (upper, lower) in enumerate(
        [
            (n_hi, n_hi), (ft_hi, ft_hi), (nt_hi, nt_hi), (f_hi, f_hi), (c_hi, c_hi),
            (c_lo, jnp.zeros_like(c_lo)),
        ]
    ):
        main_w[pl.ds(0, 128), pl.ds(128 * i, 128)] = upper
        main_w[pl.ds(128, 128), pl.ds(128 * i, 128)] = lower
    for i, (upper, lower) in enumerate([(n_lo, f_lo), (ft_lo, nt_lo)]):
        mix_w[pl.ds(0, 128), pl.ds(128 * i, 128)] = upper
        mix_w[pl.ds(128, 128), pl.ds(128 * i, 128)] = lower
    eye = lax.broadcasted_iota(jnp.int32, (128, 128), 0) == lax.broadcasted_iota(
        jnp.int32, (128, 128), 1
    )
    diag = jnp.sum(jnp.where(eye, cell_m, 0.0), axis=0, keepdims=True)
    y[:, pl.ds(0, stride), :] = jnp.zeros((5, stride, 128), F32)
    y[:, pl.ds(stride + total, stride), :] = jnp.zeros((5, stride, 128), F32)
    for ref in (strip1, strip2, strip3):
        ref[pl.ds(8 * stride, stride), :] = jnp.zeros((stride, 128), F32)
    c_x[pl.ds(c_total, stride), :] = jnp.zeros((stride, 128), F32)
    x[pl.ds(inner, right + stride), :] = jnp.zeros((right + stride, 128), F32)
    wide_a[pl.ds(inner, right), :] = jnp.zeros((right, 128), F32)
    c_own[...] = jnp.zeros_like(c_own)
    res[pl.ds(right + cap, stride), :] = jnp.zeros((stride, 128), F32)

    def products(field, first, size):
        hi, lo = split(field[pl.ds(first, size), :])
        pair = jnp.concatenate([hi, lo], 1)
        ahead = field[pl.ds(first + stride - 1, size), :].astype(BF16)
        rows = pl.ds(stride + first, size)
        part = jnp.dot(
            pair, main_w[:, pl.ds(0, 256)], preferred_element_type=F32
        ) + jnp.dot(
            jnp.concatenate([hi, ahead], 1), mix_w[...], preferred_element_type=F32
        )
        y[1, rows, :] = part[:, :128]
        y[4, rows, :] = part[:, 128:]
        part = jnp.dot(pair, main_w[:, pl.ds(256, 256)], preferred_element_type=F32)
        y[2, rows, :] = part[:, :128]
        y[3, rows, :] = part[:, 128:]
        part = jnp.dot(pair, main_w[:, pl.ds(512, 256)], preferred_element_type=F32)
        y[0, rows, :] = part[:, :128] + part[:, 128:]

    def residual(field, coefs, source, low, high, shift=0):
        size = high - low
        products(field, low - stride, size + 2 * stride)
        row = stride + low
        wide = pl.ds(low + shift, size)
        return source[wide, :] - (
            coefs[wide, :] * field[pl.ds(low, size), :]
            + y[0, pl.ds(row, size), :]
            + y[1, pl.ds(row + 1, size), :]
            + y[2, pl.ds(row - 1, size), :]
            + y[3, pl.ds(row + stride, size), :]
            + y[4, pl.ds(row - stride, size), :]
        )

    def improve(field, update, coefs, scale, source, low, high, keep, gain):
        rows = pl.ds(low, high - low)
        step = gain * scale[rows, :] * residual(field, coefs, source, low, high)
        if keep is not None:
            step = keep * update[rows, :] + step
        update[rows, :] = step
        field[rows, :] = field[rows, :] + step

    pairs = weights_of()
    has_prev = me > 0
    has_next = me < n - 1

    own = pl.ds(left, cap)
    own_rows = rows_of(0, cap) < live
    own_j = jnp.where(own_rows, 1.0 / (wide_a[own, :] + diag), 0.0)
    own_b = jnp.where(own_rows, b_own[...], 0.0)
    wide_j[own, :] = own_j
    wide_b[own, :] = own_b
    wide_j[pl.ds(inner, right), :] = jnp.zeros((right, 128), F32)
    wide_b[pl.ds(inner, right), :] = jnp.zeros((right, 128), F32)
    first = own_j * own_b * (1.0 / CENTER)
    x[own, :] = first
    d[own, :] = first
    strip1[pl.ds(left, 2 * stride), :] = first[: 2 * stride]
    improve(x, d, wide_a, wide_j, wide_b, left + stride, inner, *pairs[0])
    strip2[pl.ds(left, 2 * stride), :] = x[pl.ds(left + stride, 2 * stride), :]
    strip_d[pl.ds(left, 2 * stride), :] = d[pl.ds(left + stride, 2 * stride), :]
    improve(x, d, wide_a, wide_j, wide_b, left + 2 * stride, inner, *pairs[1])
    strip3[pl.ds(left, 2 * stride), :] = x[pl.ds(left + 2 * stride, 2 * stride), :]
    res[pl.ds(2 * right, cap - right), :] = residual(
        x, wide_a, wide_b, left + right, inner
    )

    @pl.when(jnp.logical_not(early))
    def _():
        start(halo[0])

    loads[6].wait()
    for i in range(8):
        m = prolong[i]
        high, low = split(m)
        pro_w[pl.ds(0, 128), pl.ds(128 * i, 128)] = high
        pro_w[pl.ds(128, 128), pl.ds(128 * i, 128)] = high
        pro_low[:, pl.ds(128 * i, 128)] = low
        high, low = split(jnp.transpose(m))
        for k in range(2):
            rest_w[pl.ds(256 * i + 128 * k, 128), pl.ds(0, 128)] = high
            rest_w[pl.ds(256 * i + 128 * k, 128), pl.ds(128, 128)] = low

    low_limit = jnp.where(has_prev, 0, left)
    left_rows = rows_of(0, left) >= low_limit
    received(metas[0])
    start(metas[1])
    start(halo[1])
    for c, other in ((metas[2], metas[3]), (metas[4], metas[5])):
        received(c)
        start(other)
    for i in range(cap // 128):
        a_left[pl.ds(128 * i, 128), :] = columns(meta_in[0, pl.ds(i, 1), :])
    n1 = lax.div(count(at(-1)), 8)
    a_low = jnp.where(left_rows, a_left[pl.ds(8 * (n1 - left // 8), left), :], 0.0)
    wide_a[pl.ds(0, left), :] = a_low
    j_low = jnp.where(left_rows, 1.0 / (jnp.where(left_rows, a_low, 16.0) + diag), 0.0)
    wide_j[pl.ds(0, left), :] = j_low

    received(halo[0])
    b_low = jnp.where(left_rows, ghost_low[...], 0.0)
    wide_b[pl.ds(0, left), :] = b_low
    strip1[pl.ds(0, left), :] = j_low * b_low * (1.0 / CENTER)
    low, high = stride, 7 * stride
    middle = pl.ds(low, high - low)
    keep, gain = pairs[0]
    step = gain * wide_j[middle, :] * residual(strip1, wide_a, wide_b, low, high)
    step = keep * strip1[middle, :] + step
    strip_d[pl.ds(0, left), :] = step
    strip2[pl.ds(0, left), :] = strip1[middle, :] + step
    keep, gain = pairs[1]
    step = gain * wide_j[pl.ds(low + stride, left), :] * residual(
        strip2, wide_a, wide_b, low, high, stride
    )
    step = keep * strip_d[middle, :] + step
    strip3[pl.ds(0, left), :] = strip2[middle, :] + step
    res[pl.ds(0, left), :] = residual(strip3, wide_a, wide_b, low, high, 2 * stride)

    acc = jnp.zeros((base, 256), F32)
    for i in range(8):
        hi, lo = split(res[pl.ds(i, base, stride=8), :])
        acc = acc + jnp.dot(
            jnp.concatenate([hi, lo], 1), rest_w[pl.ds(256 * i, 256), :],
            preferred_element_type=F32,
        )
    front = c_cap + 8
    c_own[pl.ds(front, base), :] = acc[:, :128] + acc[:, 128:]
    c_tail[...] = c_own[pl.ds(8 + c_live, c_cap), :]
    coarse = [
        remote(c_tail, l1.at[pl.ds(8, c_cap)], c_send, c_recv, 0),
        remote(c_own.at[pl.ds(front, base)], r1.at[pl.ds(40, base)], c_send, c_recv, 1),
        remote(c_tail.at[pl.ds(c_cap - 32, 32)], l2.at[pl.ds(8, 32)], c_send, c_recv, 2),
        remote(c_own.at[pl.ds(front, 56)], r2.at[pl.ds(72, 56)], c_send, c_recv, 3),
        remote(c_own.at[pl.ds(front, 24)], r3.at[pl.ds(104, 24)], c_send, c_recv, 5, 4),
    ]
    for c in coarse:
        start(c)
    x[pl.ds(2 * stride, left), :] = strip3[pl.ds(0, left), :]
    x_head[...] = x[pl.ds(left - 2 * stride, 5 * stride), :]
    halo_x = remote(x_head, x_high.at[pl.ds(half, 5 * stride)], x_send, x_recv, 1, 0)
    start(halo_x)

    for c in metas[1::2]:
        received(c)
    for i in range(2):
        a_high[pl.ds(half + 128 * i, 128), :] = columns(meta_in[1, pl.ds(i, 1), :])
    for i, (ref, at_row, top, size) in enumerate(
        [
            (k1, 16, 128 - c_cap, c_cap), (q1, 32, 0, c_cap),
            (k2, 0, 128 - 48, 48), (q2, 64, 0, 48),
            (k3, 0, 128 - 16, 16), (q3, 96, 0, 16),
        ]
    ):
        ref[pl.ds(at_row, size), :] = columns(meta_in[i, pl.ds(4, 1), :])[top : top + size]
    received(halo[1])
    shift = 8 * (cap // 8 - c_live)
    index = rows_of(half, more)
    limit = live + jnp.where(has_next, right, 0)
    late = pl.ds(left + half, more)
    old = index < live
    new = index < limit
    late_a = jnp.where(
        new, jnp.where(old, wide_a[late, :], a_high[pl.ds(shift, more), :]), 0.0
    )
    wide_a[late, :] = late_a
    wide_j[late, :] = jnp.where(new, 1.0 / (jnp.where(new, late_a, 16.0) + diag), 0.0)
    wide_b[late, :] = jnp.where(
        new, jnp.where(old, wide_b[late, :], ghost_high[pl.ds(shift, more), :]), 0.0
    )

    n2 = lax.div(count(at(-2)), 8)
    p1 = lax.div(count(at(1)), 8)
    p2 = lax.div(count(at(2)), 8)
    e2 = base - n1
    e3 = e2 - n2
    s1 = base + c_live
    s2 = s1 + p1
    s3 = s2 + p2
    reach = c_cap + edge
    c_low = jnp.maximum(
        base - reach, jnp.where(me >= 3, 0, jnp.where(me == 2, e3, jnp.where(me == 1, e2, base)))
    )
    c_high = jnp.minimum(
        s1 + reach,
        jnp.where(
            me + 3 < n, s3 + reach,
            jnp.where(me + 3 == n, s3, jnp.where(me + 2 == n, s2, s1)),
        ),
    )

    def zeros(rows):
        return jnp.zeros((rows, 128), F32)

    r = rows_of(0, base)
    v2 = jnp.concatenate([k2[pl.ds(48 - e2, 48), :], zeros(base - 48)], 0)
    v3 = jnp.concatenate([k3[pl.ds(16 - e3, 16), :], zeros(base - 16)], 0)
    value = jnp.where(r >= e2, k1[...], jnp.where(r >= e3, v2, v3))
    c_a[pl.ds(0, base), :] = jnp.where(r >= c_low, value, 0.0)
    r = rows_of(base, c_cap + base)
    v0 = jnp.concatenate([mean, zeros(base)], 0)
    v1 = jnp.concatenate([zeros(32), q1[pl.ds(c_cap - c_live, 112), :]], 0)
    v2 = jnp.concatenate([zeros(64), q2[pl.ds(208 - s2, 80), :]], 0)
    v3 = jnp.concatenate([zeros(96), q3[pl.ds(272 - s3, 48), :]], 0)
    value = jnp.where(r < s1, v0, jnp.where(r < s2, v1, jnp.where(r < s3, v2, v3)))
    c_a[pl.ds(base, c_cap + base), :] = jnp.where(r < c_high, value, 0.0)
    r = rows_of(0, c_total)
    c_live_rows = (r >= c_low) & (r < c_high)
    c_j[...] = jnp.where(
        c_live_rows, 1.0 / (jnp.where(c_live_rows, c_a[...], 16.0) + diag), 0.0
    )

    for c in coarse:
        received(c)
    o1 = s1 - edge
    o2 = s2 - edge
    o3 = s3 - edge
    t1 = jnp.where(me == n - 1, c_total, o1)
    t2 = jnp.where(me == n - 2, c_total, o2)
    t3 = jnp.where(me == n - 3, c_total, o3)
    f2 = e2 - edge
    r = rows_of(0, front)
    v1 = l1[pl.ds(4, front), :]
    v2 = jnp.concatenate([l2[pl.ds(40 - f2, 40), :], zeros(front - 40)], 0)
    value = jnp.where(
        r >= base - edge, c_own[pl.ds(4, front), :], jnp.where(r >= f2, v1, v2)
    )
    c_b[pl.ds(0, front), :] = jnp.where(r >= c_low, value, 0.0)
    r = rows_of(front, c_total - front)
    v0 = jnp.concatenate([c_own[pl.ds(front + 4, base), :], zeros(front)], 0)
    v1 = jnp.concatenate([zeros(24), r1[pl.ds(136 - o1, 128), :]], 0)
    v2 = jnp.concatenate([zeros(56), r2[pl.ds(200 - o2, 96), :]], 0)
    v3 = jnp.concatenate([zeros(88), r3[pl.ds(264 - o3, 64), :]], 0)
    value = jnp.where(r < t1, v0, jnp.where(r < t2, v1, jnp.where(r < t3, v2, v3)))
    c_b[pl.ds(front, c_total - front), :] = jnp.where(
        (r >= c_low) & (r < c_high), value, 0.0
    )
    first = c_j[...] * c_b[...] * (1.0 / CENTER)
    c_x[pl.ds(0, c_total), :] = first
    c_d[...] = first
    for i, (keep, gain) in enumerate(pairs):
        low = stride * (i + 1)
        improve(c_x, c_d, c_a, c_j, c_b, low, c_total - low, keep, gain)

    received(halo_x)
    index = rows_of(left, cap + right - left)
    keep_x = live - jnp.where(has_next, 2 * stride, 0)
    late = pl.ds(2 * left, cap + right - left)
    x[late, :] = jnp.where(
        index < limit,
        jnp.where(index < keep_x, x[late, :], x_high[pl.ds(shift, cap + right - left), :]),
        0.0,
    )
    rows = c_cap + 2 * edge
    hi, lo = split(c_x[pl.ds(base - edge, rows), :])
    pair = jnp.concatenate([hi, lo], 1)
    for begin in range(0, 1024, 256):
        part = jnp.dot(
            pair, pro_w[:, pl.ds(begin, 256)], preferred_element_type=F32
        ) + jnp.dot(hi, pro_low[:, pl.ds(begin, 256)], preferred_element_type=F32)
        for k in range(2):
            where = pl.ds(right + begin // 128 + k, rows, stride=8)
            x[where, :] = x[where, :] + part[:, 128 * k : 128 * k + 128]

    low, high = left - 2 * stride, total - stride
    improve(x, d, wide_a, wide_j, wide_b, low, high, None, 1.0 / CENTER)
    for keep, gain in pairs:
        low, high = low + stride, high - stride
        improve(x, d, wide_a, wide_j, wide_b, low, high, keep, gain)
    out_ref[...] = jnp.where(own_rows, x[own, :], 0.0)
    for c in halo + metas + coarse + [halo_x]:
        sent(c)


def shards(n, lanes, right_side, cell_coef, fine_count, cell_matrix, face_near, face_far, prolong):
    cap = right_side.shape[0]
    stride = cap // 16
    left = 6 * stride
    right = 3 * stride
    total = left + cap + right
    c_cap = cap // 8
    base = c_cap + 16
    c_total = 2 * base + c_cap
    half = cap // 2

    def vmem(*shape, dtype=F32):
        return pltpu.VMEM(shape, dtype)

    scratch = [
        pltpu.SMEM(fine_count.shape, jnp.int32), vmem(cap, 128), vmem(4, 128),
        vmem(128, 128), vmem(128, 128), vmem(128, 128), vmem(8, 128, 128),
        vmem(left, 128), vmem(left, 128), vmem(cap + right, 128), vmem(8, 128),
        vmem(6, 8, 128),
        vmem(cap, 128), vmem(cap + right, 128), vmem(total, 128), vmem(total, 128),
        vmem(total, 128), vmem(total + stride, 128), vmem(total, 128),
        vmem(5, total + 2 * stride, 128), vmem(cap + right + stride, 128),
        vmem(9 * stride, 128), vmem(9 * stride, 128), vmem(9 * stride, 128),
        vmem(8 * stride, 128),
        vmem(256, 768, dtype=BF16), vmem(256, 256, dtype=BF16),
        vmem(2048, 256, dtype=BF16),
        vmem(256, 1024, dtype=BF16), vmem(128, 1024, dtype=BF16),
        vmem(160, 128), vmem(c_cap, 128), vmem(2 * c_cap, 128),
        vmem(88, 128), vmem(80, 128), vmem(168, 128), vmem(168, 128), vmem(168, 128),
    ]
    scratch += [vmem(base, 128)] * 3 + [vmem(base + c_cap, 128)] * 3
    scratch += [vmem(c_total, 128)] * 3 + [vmem(c_total + stride, 128), vmem(c_total, 128)]
    scratch += [vmem(5 * stride, 128), vmem(half + 416, 128)]
    dma = pltpu.SemaphoreType.DMA
    scratch += [dma((7,)), dma((2,)), dma((2,)), dma((6,)), dma((6,)), dma((5,)), dma((5,))]
    scratch += [dma((1,)), dma((1,))]
    return pl.pallas_call(
        functools.partial(cycle, n, lanes, cap),
        out_shape=jax.ShapeDtypeStruct(right_side.shape, F32),
        in_specs=[pl.BlockSpec(memory_space=pltpu.MemorySpace.HBM)] * 7,
        out_specs=pl.BlockSpec(memory_space=pltpu.VMEM),
        scratch_shapes=scratch,
        compiler_params=pltpu.CompilerParams(
            collective_id=0, has_side_effects=True, vmem_limit_bytes=32 * 2**20
        ),
        name="cycle",
    )(
        *(
            pltpu.with_memory_space_constraint(v, pltpu.MemorySpace.HBM)
            for v in (
                fine_count, right_side, cell_coef.reshape(4, 128), cell_matrix, face_near,
                face_far, prolong,
            )
        )
    )


def solution(mesh):
    placed = (P(("sfc", "lvl"), None), P(("sfc", "lvl")), P(), P(), P(), P(), P())
    lanes = mesh.shape["lvl"]
    n = mesh.shape["sfc"] * lanes
    return jax.shard_map(
        functools.partial(shards, n, lanes),
        mesh=mesh, in_specs=placed, out_specs=P(("sfc", "lvl"), None), check_vma=False,
    )
```

```python
import functools

import jax
import jax.numpy as jnp
from jax import lax
from jax.experimental import pallas as pl
from jax.experimental.pallas import tpu as pltpu
from jax.sharding import PartitionSpec as P

DEG = 3
CENTER = 1.025
RADIUS = 0.775
STEPS = (1, -1, 2, -2, 3, -3)
F32 = jnp.float32
BF16 = jnp.bfloat16


def weights_of():
    ratio = CENTER / RADIUS
    prev = 1.0 / ratio
    pairs = []
    for _ in range(DEG - 1):
        new = 1.0 / (2.0 * ratio - prev)
        pairs.append((new * prev, 2.0 * new / RADIUS))
        prev = new
    return pairs


def split(x):
    high = x.astype(BF16)
    low = (x - high.astype(F32)).astype(BF16)
    return high, low


def rows_of(start, size):
    return start + lax.broadcasted_iota(jnp.int32, (size, 128), 0)


def columns(row):
    return jnp.transpose(jnp.broadcast_to(row, (128, 128)))


def cycle(
    n, lanes, cap,
    counts_hbm, b_hbm, coef_hbm, cell_hbm, near_hbm, far_hbm, prolong_hbm,
    out_ref,
    counts, b_own, coef, cell, near, far, prolong,
    tail, ghost_low, ghost_high, meta, meta_in, coef_in,
    a_left, a_high, wide_b, wide_a, wide_j, x, d, y, res,
    strip1, strip2, strip3, strip_d,
    main_w, mix_w, rest_w, pro_w, pro_low,
    c_own, c_tail, c_coef, l1, l2, r1, r2, r3, k1, k2, k3, q1, q2, q3,
    c_b, c_a, c_j, c_x, c_d, x_head, x_high,
    local_sem, b_send, b_recv, m_send, m_recv, c_send, c_recv, x_send, x_recv,
):
    stride = cap // 16
    left = 6 * stride
    right = 3 * stride
    total = left + cap + right
    inner = left + cap
    c_cap = cap // 8
    edge = right // 8
    base = c_cap + 16
    c_total = base + c_cap + base
    half = cap // 2
    more = half + right
    me = lax.axis_index("sfc") * lanes + lax.axis_index("lvl")

    def at(step):
        return lax.rem(me + (step + n), n)

    def device(step):
        t = at(step)
        return (lax.div(t, lanes), lax.rem(t, lanes))

    def exists(step):
        return me >= -step if step < 0 else me < n - step

    barrier = pltpu.get_barrier_semaphore()

    def signal(step):
        @pl.when(exists(step))
        def _():
            pl.semaphore_signal(
                barrier, inc=1, device_id=device(step), device_id_type=pl.DeviceIdType.MESH
            )

    for step in (-1, -2, -3):
        signal(step)
    loads = [
        pltpu.make_async_copy(src, dst, local_sem.at[i])
        for i, (src, dst) in enumerate(
            [
                (counts_hbm, counts), (coef_hbm, coef), (b_hbm, b_own), (cell_hbm, cell),
                (near_hbm, near), (far_hbm, far), (prolong_hbm, prolong),
            ]
        )
    ]
    for c in loads:
        c.start()

    def remote(src, dst, send, recv, slot, sem=None):
        sem = slot if sem is None else sem
        copy = pltpu.make_async_remote_copy(
            src_ref=src, dst_ref=dst, send_sem=send.at[sem], recv_sem=recv.at[sem],
            device_id=device(STEPS[slot]), device_id_type=pl.DeviceIdType.MESH,
        )
        return copy, STEPS[slot]

    def start(pair):
        @pl.when(exists(pair[1]))
        def _():
            pair[0].start()

    def received(pair):
        @pl.when(exists(-pair[1]))
        def _():
            pair[0].wait_recv()

    def sent(pair):
        @pl.when(exists(pair[1]))
        def _():
            pair[0].wait_send()

    loads[0].wait()
    loads[1].wait()

    def count(t):
        return jnp.minimum(jnp.maximum(counts[t], half), cap)

    live = count(me)
    c_live = lax.div(live, 8)
    loads[2].wait()
    tail[...] = b_own[pl.ds(8 * (c_live - left // 8), left), :]

    @pl.when(me < n - 1)
    def _():
        pl.semaphore_wait(barrier, jnp.minimum(n - 1 - me, 3))

    halo = [
        remote(tail, ghost_low, b_send, b_recv, 0),
        remote(b_own.at[pl.ds(0, right)], ghost_high.at[pl.ds(half, right)], b_send, b_recv, 1),
    ]
    raw = remote(coef, coef_in, b_send, b_recv, 0, 2)
    start(raw)
    early = lax.rem(lax.axis_index("sfc"), 2) == 1

    @pl.when(early)
    def _():
        start(halo[0])

    for i in range(cap // 128):
        wide_a[pl.ds(left + 128 * i, 128), :] = columns(coef[pl.ds(i, 1), :])
    mean = wide_a[pl.ds(left, c_cap, stride=8), :]
    for c in range(1, 8):
        mean = mean + wide_a[pl.ds(left + c, c_cap, stride=8), :]
    mean = mean * 0.125
    c_coef[pl.ds(0, c_cap), :] = jnp.zeros((c_cap, 128), F32)
    c_coef[pl.ds(c_cap, c_cap), :] = mean
    both = jnp.concatenate([mean, c_coef[pl.ds(c_live, c_cap), :]], 0)
    meta[pl.ds(0, 4), :] = coef[...]
    meta[pl.ds(4, 4), :] = jnp.transpose(both)[0:4, :]
    metas = [
        remote(meta, meta_in.at[i], m_send, m_recv, i) for i in range(len(STEPS))
    ]
    for c in metas[::2]:
        start(c)

    for c in loads[3:6]:
        c.wait()
    cell_m = cell[...]
    parts = [cell_m, -near[...], -jnp.transpose(near[...]), -far[...], -jnp.transpose(far[...])]
    parts = [split(m) for m in parts]
    (c_hi, c_lo), (n_hi, n_lo), (nt_hi, nt_lo), (f_hi, f_lo), (ft_hi, ft_lo) = parts
    for i, (upper, lower) in enumerate(
        [
            (n_hi, n_hi), (ft_hi, ft_hi), (nt_hi, nt_hi), (f_hi, f_hi), (c_hi, c_hi),
            (c_lo, jnp.zeros_like(c_lo)),
        ]
    ):
        main_w[pl.ds(0, 128), pl.ds(128 * i, 128)] = upper
        main_w[pl.ds(128, 128), pl.ds(128 * i, 128)] = lower
    for i, (upper, lower) in enumerate([(n_lo, f_lo), (ft_lo, nt_lo)]):
        mix_w[pl.ds(0, 128), pl.ds(128 * i, 128)] = upper
        mix_w[pl.ds(128, 128), pl.ds(128 * i, 128)] = lower
    eye = lax.broadcasted_iota(jnp.int32, (128, 128), 0) == lax.broadcasted_iota(
        jnp.int32, (128, 128), 1
    )
    diag = jnp.sum(jnp.where(eye, cell_m, 0.0), axis=0, keepdims=True)
    y[:, pl.ds(0, stride), :] = jnp.zeros((5, stride, 128), F32)
    y[:, pl.ds(stride + total, stride), :] = jnp.zeros((5, stride, 128), F32)
    for ref in (strip1, strip2, strip3):
        ref[pl.ds(8 * stride, stride), :] = jnp.zeros((stride, 128), F32)
    c_x[pl.ds(c_total, stride), :] = jnp.zeros((stride, 128), F32)
    x[pl.ds(inner, right + stride), :] = jnp.zeros((right + stride, 128), F32)
    wide_a[pl.ds(inner, right), :] = jnp.zeros((right, 128), F32)
    c_own[...] = jnp.zeros_like(c_own)
    res[pl.ds(right + cap, stride), :] = jnp.zeros((stride, 128), F32)

    def products(field, first, size):
        hi, lo = split(field[pl.ds(first, size), :])
        pair = jnp.concatenate([hi, lo], 1)
        ahead = field[pl.ds(first + stride - 1, size), :].astype(BF16)
        rows = pl.ds(stride + first, size)
        part = jnp.dot(
            pair, main_w[:, pl.ds(0, 256)], preferred_element_type=F32
        ) + jnp.dot(
            jnp.concatenate([hi, ahead], 1), mix_w[...], preferred_element_type=F32
        )
        y[1, rows, :] = part[:, :128]
        y[4, rows, :] = part[:, 128:]
        part = jnp.dot(pair, main_w[:, pl.ds(256, 256)], preferred_element_type=F32)
        y[2, rows, :] = part[:, :128]
        y[3, rows, :] = part[:, 128:]
        part = jnp.dot(pair, main_w[:, pl.ds(512, 256)], preferred_element_type=F32)
        y[0, rows, :] = part[:, :128] + part[:, 128:]

    def residual(field, coefs, source, low, high, shift=0):
        size = high - low
        products(field, low - stride, size + 2 * stride)
        row = stride + low
        wide = pl.ds(low + shift, size)
        return source[wide, :] - (
            coefs[wide, :] * field[pl.ds(low, size), :]
            + y[0, pl.ds(row, size), :]
            + y[1, pl.ds(row + 1, size), :]
            + y[2, pl.ds(row - 1, size), :]
            + y[3, pl.ds(row + stride, size), :]
            + y[4, pl.ds(row - stride, size), :]
        )

    def improve(field, update, coefs, scale, source, low, high, keep, gain):
        rows = pl.ds(low, high - low)
        step = gain * scale[rows, :] * residual(field, coefs, source, low, high)
        if keep is not None:
            step = keep * update[rows, :] + step
        update[rows, :] = step
        field[rows, :] = field[rows, :] + step

    pairs = weights_of()
    has_prev = me > 0
    has_next = me < n - 1

    own = pl.ds(left, cap)
    own_rows = rows_of(0, cap) < live
    own_j = jnp.where(own_rows, 1.0 / (wide_a[own, :] + diag), 0.0)
    own_b = jnp.where(own_rows, b_own[...], 0.0)
    wide_j[own, :] = own_j
    wide_b[own, :] = own_b
    wide_j[pl.ds(inner, right), :] = jnp.zeros((right, 128), F32)
    wide_b[pl.ds(inner, right), :] = jnp.zeros((right, 128), F32)
    first = own_j * own_b * (1.0 / CENTER)
    x[own, :] = first
    d[own, :] = first
    strip1[pl.ds(left, 2 * stride), :] = first[: 2 * stride]
    improve(x, d, wide_a, wide_j, wide_b, left + stride, inner, *pairs[0])
    strip2[pl.ds(left, 2 * stride), :] = x[pl.ds(left + stride, 2 * stride), :]
    strip_d[pl.ds(left, 2 * stride), :] = d[pl.ds(left + stride, 2 * stride), :]
    improve(x, d, wide_a, wide_j, wide_b, left + 2 * stride, inner, *pairs[1])
    strip3[pl.ds(left, 2 * stride), :] = x[pl.ds(left + 2 * stride, 2 * stride), :]
    res[pl.ds(2 * right, cap - right), :] = residual(
        x, wide_a, wide_b, left + right, inner
    )

    @pl.when(jnp.logical_not(early))
    def _():
        start(halo[0])

    loads[6].wait()
    for i in range(8):
        m = prolong[i]
        high, low = split(m)
        pro_w[pl.ds(0, 128), pl.ds(128 * i, 128)] = high
        pro_w[pl.ds(128, 128), pl.ds(128 * i, 128)] = high
        pro_low[:, pl.ds(128 * i, 128)] = low
        high, low = split(jnp.transpose(m))
        for k in range(2):
            rest_w[pl.ds(256 * i + 128 * k, 128), pl.ds(0, 128)] = high
            rest_w[pl.ds(256 * i + 128 * k, 128), pl.ds(128, 128)] = low

    low_limit = jnp.where(has_prev, 0, left)
    left_rows = rows_of(0, left) >= low_limit
    received(raw)
    start(metas[1])
    start(halo[1])
    for i in range(cap // 128):
        a_left[pl.ds(128 * i, 128), :] = columns(coef_in[pl.ds(i, 1), :])
    n1 = lax.div(count(at(-1)), 8)
    a_low = jnp.where(left_rows, a_left[pl.ds(8 * (n1 - left // 8), left), :], 0.0)
    wide_a[pl.ds(0, left), :] = a_low
    j_low = jnp.where(left_rows, 1.0 / (jnp.where(left_rows, a_low, 16.0) + diag), 0.0)
    wide_j[pl.ds(0, left), :] = j_low

    received(halo[0])
    b_low = jnp.where(left_rows, ghost_low[...], 0.0)
    wide_b[pl.ds(0, left), :] = b_low
    strip1[pl.ds(0, left), :] = j_low * b_low * (1.0 / CENTER)
    low, high = stride, 7 * stride
    middle = pl.ds(low, high - low)
    keep, gain = pairs[0]
    step = gain * wide_j[middle, :] * residual(strip1, wide_a, wide_b, low, high)
    step = keep * strip1[middle, :] + step
    strip_d[pl.ds(0, left), :] = step
    strip2[pl.ds(0, left), :] = strip1[middle, :] + step
    keep, gain = pairs[1]
    step = gain * wide_j[pl.ds(low + stride, left), :] * residual(
        strip2, wide_a, wide_b, low, high, stride
    )
    step = keep * strip_d[middle, :] + step
    strip3[pl.ds(0, left), :] = strip2[middle, :] + step
    res[pl.ds(0, left), :] = residual(strip3, wide_a, wide_b, low, high, 2 * stride)

    acc = jnp.zeros((base, 256), F32)
    for i in range(8):
        hi, lo = split(res[pl.ds(i, base, stride=8), :])
        acc = acc + jnp.dot(
            jnp.concatenate([hi, lo], 1), rest_w[pl.ds(256 * i, 256), :],
            preferred_element_type=F32,
        )
    front = c_cap + 8
    c_own[pl.ds(front, base), :] = acc[:, :128] + acc[:, 128:]
    c_tail[...] = c_own[pl.ds(8 + c_live, c_cap), :]
    coarse = [
        remote(c_tail, l1.at[pl.ds(8, c_cap)], c_send, c_recv, 0),
        remote(c_own.at[pl.ds(front, base)], r1.at[pl.ds(40, base)], c_send, c_recv, 1),
        remote(c_tail.at[pl.ds(c_cap - 32, 32)], l2.at[pl.ds(8, 32)], c_send, c_recv, 2),
        remote(c_own.at[pl.ds(front, 56)], r2.at[pl.ds(72, 56)], c_send, c_recv, 3),
        remote(c_own.at[pl.ds(front, 24)], r3.at[pl.ds(104, 24)], c_send, c_recv, 5, 4),
    ]
    for c in (coarse[0], coarse[2], coarse[1]):
        start(c)
    x[pl.ds(2 * stride, left), :] = strip3[pl.ds(0, left), :]
    x_head[...] = x[pl.ds(left - 2 * stride, 5 * stride), :]
    halo_x = remote(x_head, x_high.at[pl.ds(half, 5 * stride)], x_send, x_recv, 1, 0)
    start(halo_x)
    for c, other, rows in ((metas[2], metas[3], coarse[3]), (metas[4], metas[5], coarse[4])):
        received(c)
        start(other)
        start(rows)
    received(metas[0])

    for c in metas[1::2]:
        received(c)
    for i in range(2):
        a_high[pl.ds(half + 128 * i, 128), :] = columns(meta_in[1, pl.ds(i, 1), :])
    for i, (ref, at_row, top, size) in enumerate(
        [
            (k1, 16, 128 - c_cap, c_cap), (q1, 32, 0, c_cap),
            (k2, 0, 128 - 48, 48), (q2, 64, 0, 48),
            (k3, 0, 128 - 16, 16), (q3, 96, 0, 16),
        ]
    ):
        ref[pl.ds(at_row, size), :] = columns(meta_in[i, pl.ds(4, 1), :])[top : top + size]
    received(halo[1])
    shift = 8 * (cap // 8 - c_live)
    index = rows_of(half, more)
    limit = live + jnp.where(has_next, right, 0)
    late = pl.ds(left + half, more)
    old = index < live
    new = index < limit
    late_a = jnp.where(
        new, jnp.where(old, wide_a[late, :], a_high[pl.ds(shift, more), :]), 0.0
    )
    wide_a[late, :] = late_a
    wide_j[late, :] = jnp.where(new, 1.0 / (jnp.where(new, late_a, 16.0) + diag), 0.0)
    wide_b[late, :] = jnp.where(
        new, jnp.where(old, wide_b[late, :], ghost_high[pl.ds(shift, more), :]), 0.0
    )

    n2 = lax.div(count(at(-2)), 8)
    p1 = lax.div(count(at(1)), 8)
    p2 = lax.div(count(at(2)), 8)
    e2 = base - n1
    e3 = e2 - n2
    s1 = base + c_live
    s2 = s1 + p1
    s3 = s2 + p2
    reach = c_cap + edge
    c_low = jnp.maximum(
        base - reach, jnp.where(me >= 3, 0, jnp.where(me == 2, e3, jnp.where(me == 1, e2, base)))
    )
    c_high = jnp.minimum(
        s1 + reach,
        jnp.where(
            me + 3 < n, s3 + reach,
            jnp.where(me + 3 == n, s3, jnp.where(me + 2 == n, s2, s1)),
        ),
    )

    def zeros(rows):
        return jnp.zeros((rows, 128), F32)

    r = rows_of(0, base)
    v2 = jnp.concatenate([k2[pl.ds(48 - e2, 48), :], zeros(base - 48)], 0)
    v3 = jnp.concatenate([k3[pl.ds(16 - e3, 16), :], zeros(base - 16)], 0)
    value = jnp.where(r >= e2, k1[...], jnp.where(r >= e3, v2, v3))
    c_a[pl.ds(0, base), :] = jnp.where(r >= c_low, value, 0.0)
    r = rows_of(base, c_cap + base)
    v0 = jnp.concatenate([mean, zeros(base)], 0)
    v1 = jnp.concatenate([zeros(32), q1[pl.ds(c_cap - c_live, 112), :]], 0)
    v2 = jnp.concatenate([zeros(64), q2[pl.ds(208 - s2, 80), :]], 0)
    v3 = jnp.concatenate([zeros(96), q3[pl.ds(272 - s3, 48), :]], 0)
    value = jnp.where(r < s1, v0, jnp.where(r < s2, v1, jnp.where(r < s3, v2, v3)))
    c_a[pl.ds(base, c_cap + base), :] = jnp.where(r < c_high, value, 0.0)
    r = rows_of(0, c_total)
    c_live_rows = (r >= c_low) & (r < c_high)
    c_j[...] = jnp.where(
        c_live_rows, 1.0 / (jnp.where(c_live_rows, c_a[...], 16.0) + diag), 0.0
    )

    for c in coarse:
        received(c)
    o1 = s1 - edge
    o2 = s2 - edge
    o3 = s3 - edge
    t1 = jnp.where(me == n - 1, c_total, o1)
    t2 = jnp.where(me == n - 2, c_total, o2)
    t3 = jnp.where(me == n - 3, c_total, o3)
    f2 = e2 - edge
    r = rows_of(0, front)
    v1 = l1[pl.ds(4, front), :]
    v2 = jnp.concatenate([l2[pl.ds(40 - f2, 40), :], zeros(front - 40)], 0)
    value = jnp.where(
        r >= base - edge, c_own[pl.ds(4, front), :], jnp.where(r >= f2, v1, v2)
    )
    c_b[pl.ds(0, front), :] = jnp.where(r >= c_low, value, 0.0)
    r = rows_of(front, c_total - front)
    v0 = jnp.concatenate([c_own[pl.ds(front + 4, base), :], zeros(front)], 0)
    v1 = jnp.concatenate([zeros(24), r1[pl.ds(136 - o1, 128), :]], 0)
    v2 = jnp.concatenate([zeros(56), r2[pl.ds(200 - o2, 96), :]], 0)
    v3 = jnp.concatenate([zeros(88), r3[pl.ds(264 - o3, 64), :]], 0)
    value = jnp.where(r < t1, v0, jnp.where(r < t2, v1, jnp.where(r < t3, v2, v3)))
    c_b[pl.ds(front, c_total - front), :] = jnp.where(
        (r >= c_low) & (r < c_high), value, 0.0
    )
    first = c_j[...] * c_b[...] * (1.0 / CENTER)
    c_x[pl.ds(0, c_total), :] = first
    c_d[...] = first
    for i, (keep, gain) in enumerate(pairs):
        low = stride * (i + 1)
        improve(c_x, c_d, c_a, c_j, c_b, low, c_total - low, keep, gain)

    received(halo_x)
    index = rows_of(left, cap + right - left)
    keep_x = live - jnp.where(has_next, 2 * stride, 0)
    late = pl.ds(2 * left, cap + right - left)
    x[late, :] = jnp.where(
        index < limit,
        jnp.where(index < keep_x, x[late, :], x_high[pl.ds(shift, cap + right - left), :]),
        0.0,
    )
    rows = c_cap + 2 * edge
    hi, lo = split(c_x[pl.ds(base - edge, rows), :])
    pair = jnp.concatenate([hi, lo], 1)
    for begin in range(0, 1024, 256):
        part = jnp.dot(
            pair, pro_w[:, pl.ds(begin, 256)], preferred_element_type=F32
        ) + jnp.dot(hi, pro_low[:, pl.ds(begin, 256)], preferred_element_type=F32)
        for k in range(2):
            where = pl.ds(right + begin // 128 + k, rows, stride=8)
            x[where, :] = x[where, :] + part[:, 128 * k : 128 * k + 128]

    low, high = left - 2 * stride, total - stride
    improve(x, d, wide_a, wide_j, wide_b, low, high, None, 1.0 / CENTER)
    for keep, gain in pairs:
        low, high = low + stride, high - stride
        improve(x, d, wide_a, wide_j, wide_b, low, high, keep, gain)
    out_ref[...] = jnp.where(own_rows, x[own, :], 0.0)
    for c in halo + metas + coarse + [halo_x, raw]:
        sent(c)


def shards(n, lanes, right_side, cell_coef, fine_count, cell_matrix, face_near, face_far, prolong):
    cap = right_side.shape[0]
    stride = cap // 16
    left = 6 * stride
    right = 3 * stride
    total = left + cap + right
    c_cap = cap // 8
    base = c_cap + 16
    c_total = 2 * base + c_cap
    half = cap // 2

    def vmem(*shape, dtype=F32):
        return pltpu.VMEM(shape, dtype)

    scratch = [
        pltpu.SMEM(fine_count.shape, jnp.int32), vmem(cap, 128), vmem(4, 128),
        vmem(128, 128), vmem(128, 128), vmem(128, 128), vmem(8, 128, 128),
        vmem(left, 128), vmem(left, 128), vmem(cap + right, 128), vmem(8, 128),
        vmem(6, 8, 128), vmem(4, 128),
        vmem(cap, 128), vmem(cap + right, 128), vmem(total, 128), vmem(total, 128),
        vmem(total, 128), vmem(total + stride, 128), vmem(total, 128),
        vmem(5, total + 2 * stride, 128), vmem(cap + right + stride, 128),
        vmem(9 * stride, 128), vmem(9 * stride, 128), vmem(9 * stride, 128),
        vmem(8 * stride, 128),
        vmem(256, 768, dtype=BF16), vmem(256, 256, dtype=BF16),
        vmem(2048, 256, dtype=BF16),
        vmem(256, 1024, dtype=BF16), vmem(128, 1024, dtype=BF16),
        vmem(160, 128), vmem(c_cap, 128), vmem(2 * c_cap, 128),
        vmem(88, 128), vmem(80, 128), vmem(168, 128), vmem(168, 128), vmem(168, 128),
    ]
    scratch += [vmem(base, 128)] * 3 + [vmem(base + c_cap, 128)] * 3
    scratch += [vmem(c_total, 128)] * 3 + [vmem(c_total + stride, 128), vmem(c_total, 128)]
    scratch += [vmem(5 * stride, 128), vmem(half + 416, 128)]
    dma = pltpu.SemaphoreType.DMA
    scratch += [dma((7,)), dma((3,)), dma((3,)), dma((6,)), dma((6,)), dma((5,)), dma((5,))]
    scratch += [dma((1,)), dma((1,))]
    return pl.pallas_call(
        functools.partial(cycle, n, lanes, cap),
        out_shape=jax.ShapeDtypeStruct(right_side.shape, F32),
        in_specs=[pl.BlockSpec(memory_space=pltpu.MemorySpace.HBM)] * 7,
        out_specs=pl.BlockSpec(memory_space=pltpu.VMEM),
        scratch_shapes=scratch,
        compiler_params=pltpu.CompilerParams(
            collective_id=0, has_side_effects=True, vmem_limit_bytes=32 * 2**20
        ),
        name="cycle",
    )(
        *(
            pltpu.with_memory_space_constraint(v, pltpu.MemorySpace.HBM)
            for v in (
                fine_count, right_side, cell_coef.reshape(4, 128), cell_matrix, face_near,
                face_far, prolong,
            )
        )
    )


def solution(mesh):
    placed = (P(("sfc", "lvl"), None), P(("sfc", "lvl")), P(), P(), P(), P(), P())
    lanes = mesh.shape["lvl"]
    n = mesh.shape["sfc"] * lanes
    return jax.shard_map(
        functools.partial(shards, n, lanes),
        mesh=mesh, in_specs=placed, out_specs=P(("sfc", "lvl"), None), check_vma=False,
    )
```

```python
import functools

import jax
import jax.numpy as jnp
from jax import lax
from jax.experimental import pallas as pl
from jax.experimental.pallas import tpu as pltpu
from jax.sharding import PartitionSpec as P

DEG = 3
CENTER = 1.025
RADIUS = 0.775
STEPS = (1, -1, 2, -2, 3, -3)
F32 = jnp.float32
BF16 = jnp.bfloat16


def weights_of():
    ratio = CENTER / RADIUS
    prev = 1.0 / ratio
    pairs = []
    for _ in range(DEG - 1):
        new = 1.0 / (2.0 * ratio - prev)
        pairs.append((new * prev, 2.0 * new / RADIUS))
        prev = new
    return pairs


def split(x):
    high = x.astype(BF16)
    low = (x - high.astype(F32)).astype(BF16)
    return high, low


def rows_of(start, size):
    return start + lax.broadcasted_iota(jnp.int32, (size, 128), 0)


def columns(row):
    return jnp.transpose(jnp.broadcast_to(row, (128, 128)))


def cycle(
    n, lanes, cap,
    counts_hbm, b_hbm, coef_hbm, cell_hbm, near_hbm, far_hbm, prolong_hbm,
    out_ref,
    counts, b_own, coef, cell, near, far, prolong,
    tail, ghost_low, ghost_high, meta, meta_in, coef_in,
    a_left, a_high, wide_b, wide_a, wide_j, x, d, y, res,
    strip1, strip2, strip3, strip_d,
    main_w, mix_w, rest_w, pro_w, pro_low,
    c_own, c_tail, c_coef, l1, l2, r1, r2, r3, k1, k2, k3, q1, q2, q3,
    c_b, c_a, c_j, c_x, c_d, x_head, x_high,
    local_sem, b_send, b_recv, m_send, m_recv, c_send, c_recv, x_send, x_recv,
):
    stride = cap // 16
    left = 6 * stride
    right = 3 * stride
    total = left + cap + right
    inner = left + cap
    c_cap = cap // 8
    edge = right // 8
    base = c_cap + 16
    c_total = base + c_cap + base
    half = cap // 2
    more = half + right
    me = lax.axis_index("sfc") * lanes + lax.axis_index("lvl")

    def at(step):
        return lax.rem(me + (step + n), n)

    def device(step):
        t = at(step)
        return (lax.div(t, lanes), lax.rem(t, lanes))

    def exists(step):
        return me >= -step if step < 0 else me < n - step

    barrier = pltpu.get_barrier_semaphore()

    def signal(step):
        @pl.when(exists(step))
        def _():
            pl.semaphore_signal(
                barrier, inc=1, device_id=device(step), device_id_type=pl.DeviceIdType.MESH
            )

    loads = [
        pltpu.make_async_copy(src, dst, local_sem.at[i])
        for i, (src, dst) in enumerate(
            [
                (counts_hbm, counts), (coef_hbm, coef), (b_hbm, b_own), (cell_hbm, cell),
                (near_hbm, near), (far_hbm, far), (prolong_hbm, prolong),
            ]
        )
    ]
    for c in loads:
        c.start()
    for step in (-1, -2, -3):
        signal(step)

    def remote(src, dst, send, recv, slot, sem=None):
        sem = slot if sem is None else sem
        copy = pltpu.make_async_remote_copy(
            src_ref=src, dst_ref=dst, send_sem=send.at[sem], recv_sem=recv.at[sem],
            device_id=device(STEPS[slot]), device_id_type=pl.DeviceIdType.MESH,
        )
        return copy, STEPS[slot]

    def start(pair):
        @pl.when(exists(pair[1]))
        def _():
            pair[0].start()

    def received(pair):
        @pl.when(exists(-pair[1]))
        def _():
            pair[0].wait_recv()

    def sent(pair):
        @pl.when(exists(pair[1]))
        def _():
            pair[0].wait_send()

    loads[0].wait()
    loads[1].wait()

    def count(t):
        return jnp.minimum(jnp.maximum(counts[t], half), cap)

    live = count(me)
    c_live = lax.div(live, 8)
    loads[2].wait()
    tail[...] = b_own[pl.ds(8 * (c_live - left // 8), left), :]

    @pl.when(me < n - 1)
    def _():
        pl.semaphore_wait(barrier, jnp.minimum(n - 1 - me, 3))

    halo = [
        remote(tail, ghost_low, b_send, b_recv, 0),
        remote(b_own.at[pl.ds(0, right)], ghost_high.at[pl.ds(half, right)], b_send, b_recv, 1),
    ]
    raw = remote(coef, coef_in, b_send, b_recv, 0, 2)
    start(raw)
    start(halo[0])

    for i in range(cap // 128):
        wide_a[pl.ds(left + 128 * i, 128), :] = columns(coef[pl.ds(i, 1), :])
    mean = wide_a[pl.ds(left, c_cap, stride=8), :]
    for c in range(1, 8):
        mean = mean + wide_a[pl.ds(left + c, c_cap, stride=8), :]
    mean = mean * 0.125
    c_coef[pl.ds(0, c_cap), :] = jnp.zeros((c_cap, 128), F32)
    c_coef[pl.ds(c_cap, c_cap), :] = mean
    both = jnp.concatenate([mean, c_coef[pl.ds(c_live, c_cap), :]], 0)
    meta[pl.ds(0, 4), :] = coef[...]
    meta[pl.ds(4, 4), :] = jnp.transpose(both)[0:4, :]
    metas = [
        remote(meta, meta_in.at[i], m_send, m_recv, i) for i in range(len(STEPS))
    ]
    for c in metas[::2]:
        start(c)

    for c in loads[3:6]:
        c.wait()
    cell_m = cell[...]
    parts = [cell_m, -near[...], -jnp.transpose(near[...]), -far[...], -jnp.transpose(far[...])]
    parts = [split(m) for m in parts]
    (c_hi, c_lo), (n_hi, n_lo), (nt_hi, nt_lo), (f_hi, f_lo), (ft_hi, ft_lo) = parts
    for i, (upper, lower) in enumerate(
        [
            (n_hi, n_hi), (ft_hi, ft_hi), (nt_hi, nt_hi), (f_hi, f_hi), (c_hi, c_hi),
            (c_lo, jnp.zeros_like(c_lo)),
        ]
    ):
        main_w[pl.ds(0, 128), pl.ds(128 * i, 128)] = upper
        main_w[pl.ds(128, 128), pl.ds(128 * i, 128)] = lower
    for i, (upper, lower) in enumerate([(n_lo, f_lo), (ft_lo, nt_lo)]):
        mix_w[pl.ds(0, 128), pl.ds(128 * i, 128)] = upper
        mix_w[pl.ds(128, 128), pl.ds(128 * i, 128)] = lower
    eye = lax.broadcasted_iota(jnp.int32, (128, 128), 0) == lax.broadcasted_iota(
        jnp.int32, (128, 128), 1
    )
    diag = jnp.sum(jnp.where(eye, cell_m, 0.0), axis=0, keepdims=True)
    y[:, pl.ds(0, stride), :] = jnp.zeros((5, stride, 128), F32)
    y[:, pl.ds(stride + total, stride), :] = jnp.zeros((5, stride, 128), F32)
    for ref in (strip1, strip2, strip3):
        ref[pl.ds(8 * stride, stride), :] = jnp.zeros((stride, 128), F32)
    c_x[pl.ds(c_total, stride), :] = jnp.zeros((stride, 128), F32)
    x[pl.ds(inner, right + stride), :] = jnp.zeros((right + stride, 128), F32)
    wide_a[pl.ds(inner, right), :] = jnp.zeros((right, 128), F32)
    c_own[...] = jnp.zeros_like(c_own)
    res[pl.ds(right + cap, stride), :] = jnp.zeros((stride, 128), F32)

    def products(field, first, size):
        hi, lo = split(field[pl.ds(first, size), :])
        pair = jnp.concatenate([hi, lo], 1)
        ahead = field[pl.ds(first + stride - 1, size), :].astype(BF16)
        rows = pl.ds(stride + first, size)
        part = jnp.dot(
            pair, main_w[:, pl.ds(0, 256)], preferred_element_type=F32
        ) + jnp.dot(
            jnp.concatenate([hi, ahead], 1), mix_w[...], preferred_element_type=F32
        )
        y[1, rows, :] = part[:, :128]
        y[4, rows, :] = part[:, 128:]
        part = jnp.dot(pair, main_w[:, pl.ds(256, 256)], preferred_element_type=F32)
        y[2, rows, :] = part[:, :128]
        y[3, rows, :] = part[:, 128:]
        part = jnp.dot(pair, main_w[:, pl.ds(512, 256)], preferred_element_type=F32)
        y[0, rows, :] = part[:, :128] + part[:, 128:]

    def residual(field, coefs, source, low, high, shift=0):
        size = high - low
        products(field, low - stride, size + 2 * stride)
        row = stride + low
        wide = pl.ds(low + shift, size)
        return source[wide, :] - (
            coefs[wide, :] * field[pl.ds(low, size), :]
            + y[0, pl.ds(row, size), :]
            + y[1, pl.ds(row + 1, size), :]
            + y[2, pl.ds(row - 1, size), :]
            + y[3, pl.ds(row + stride, size), :]
            + y[4, pl.ds(row - stride, size), :]
        )

    def improve(field, update, coefs, scale, source, low, high, keep, gain):
        rows = pl.ds(low, high - low)
        step = gain * scale[rows, :] * residual(field, coefs, source, low, high)
        if keep is not None:
            step = keep * update[rows, :] + step
        update[rows, :] = step
        field[rows, :] = field[rows, :] + step

    pairs = weights_of()
    has_prev = me > 0
    has_next = me < n - 1

    own = pl.ds(left, cap)
    own_rows = rows_of(0, cap) < live
    own_j = jnp.where(own_rows, 1.0 / (wide_a[own, :] + diag), 0.0)
    own_b = jnp.where(own_rows, b_own[...], 0.0)
    wide_j[own, :] = own_j
    wide_b[own, :] = own_b
    wide_j[pl.ds(inner, right), :] = jnp.zeros((right, 128), F32)
    wide_b[pl.ds(inner, right), :] = jnp.zeros((right, 128), F32)
    first = own_j * own_b * (1.0 / CENTER)
    x[own, :] = first
    d[own, :] = first
    strip1[pl.ds(left, 2 * stride), :] = first[: 2 * stride]
    improve(x, d, wide_a, wide_j, wide_b, left + stride, inner, *pairs[0])
    strip2[pl.ds(left, 2 * stride), :] = x[pl.ds(left + stride, 2 * stride), :]
    strip_d[pl.ds(left, 2 * stride), :] = d[pl.ds(left + stride, 2 * stride), :]
    improve(x, d, wide_a, wide_j, wide_b, left + 2 * stride, inner, *pairs[1])
    strip3[pl.ds(left, 2 * stride), :] = x[pl.ds(left + 2 * stride, 2 * stride), :]
    res[pl.ds(2 * right, cap - right), :] = residual(
        x, wide_a, wide_b, left + right, inner
    )

    loads[6].wait()
    for i in range(8):
        m = prolong[i]
        high, low = split(m)
        pro_w[pl.ds(0, 128), pl.ds(128 * i, 128)] = high
        pro_w[pl.ds(128, 128), pl.ds(128 * i, 128)] = high
        pro_low[:, pl.ds(128 * i, 128)] = low
        high, low = split(jnp.transpose(m))
        for k in range(2):
            rest_w[pl.ds(256 * i + 128 * k, 128), pl.ds(0, 128)] = high
            rest_w[pl.ds(256 * i + 128 * k, 128), pl.ds(128, 128)] = low

    low_limit = jnp.where(has_prev, 0, left)
    left_rows = rows_of(0, left) >= low_limit
    received(raw)
    start(metas[1])
    start(halo[1])
    for i in range(cap // 128):
        a_left[pl.ds(128 * i, 128), :] = columns(coef_in[pl.ds(i, 1), :])
    n1 = lax.div(count(at(-1)), 8)
    a_low = jnp.where(left_rows, a_left[pl.ds(8 * (n1 - left // 8), left), :], 0.0)
    wide_a[pl.ds(0, left), :] = a_low
    j_low = jnp.where(left_rows, 1.0 / (jnp.where(left_rows, a_low, 16.0) + diag), 0.0)
    wide_j[pl.ds(0, left), :] = j_low

    received(halo[0])
    b_low = jnp.where(left_rows, ghost_low[...], 0.0)
    wide_b[pl.ds(0, left), :] = b_low
    strip1[pl.ds(0, left), :] = j_low * b_low * (1.0 / CENTER)
    low, high = stride, 7 * stride
    middle = pl.ds(low, high - low)
    keep, gain = pairs[0]
    step = gain * wide_j[middle, :] * residual(strip1, wide_a, wide_b, low, high)
    step = keep * strip1[middle, :] + step
    strip_d[pl.ds(0, left), :] = step
    strip2[pl.ds(0, left), :] = strip1[middle, :] + step
    keep, gain = pairs[1]
    step = gain * wide_j[pl.ds(low + stride, left), :] * residual(
        strip2, wide_a, wide_b, low, high, stride
    )
    step = keep * strip_d[middle, :] + step
    strip3[pl.ds(0, left), :] = strip2[middle, :] + step
    res[pl.ds(0, left), :] = residual(strip3, wide_a, wide_b, low, high, 2 * stride)

    acc = jnp.zeros((base, 256), F32)
    for i in range(8):
        hi, lo = split(res[pl.ds(i, base, stride=8), :])
        acc = acc + jnp.dot(
            jnp.concatenate([hi, lo], 1), rest_w[pl.ds(256 * i, 256), :],
            preferred_element_type=F32,
        )
    front = c_cap + 8
    c_own[pl.ds(front, base), :] = acc[:, :128] + acc[:, 128:]
    c_tail[...] = c_own[pl.ds(8 + c_live, c_cap), :]
    coarse = [
        remote(c_tail, l1.at[pl.ds(8, c_cap)], c_send, c_recv, 0),
        remote(c_own.at[pl.ds(front, base)], r1.at[pl.ds(40, base)], c_send, c_recv, 1),
        remote(c_tail.at[pl.ds(c_cap - 32, 32)], l2.at[pl.ds(8, 32)], c_send, c_recv, 2),
        remote(c_own.at[pl.ds(front, 56)], r2.at[pl.ds(72, 56)], c_send, c_recv, 3),
        remote(c_own.at[pl.ds(front, 24)], r3.at[pl.ds(104, 24)], c_send, c_recv, 5, 4),
    ]
    for c in (coarse[0], coarse[2], coarse[1]):
        start(c)
    x[pl.ds(2 * stride, left), :] = strip3[pl.ds(0, left), :]
    x_head[...] = x[pl.ds(left - 2 * stride, 5 * stride), :]
    halo_x = remote(x_head, x_high.at[pl.ds(half, 5 * stride)], x_send, x_recv, 1, 0)
    start(halo_x)
    for c, other, rows in ((metas[2], metas[3], coarse[3]), (metas[4], metas[5], coarse[4])):
        received(c)
        start(other)
        start(rows)
    received(metas[0])

    for c in metas[1::2]:
        received(c)
    for i in range(2):
        a_high[pl.ds(half + 128 * i, 128), :] = columns(meta_in[1, pl.ds(i, 1), :])
    for i, (ref, at_row, top, size) in enumerate(
        [
            (k1, 16, 128 - c_cap, c_cap), (q1, 32, 0, c_cap),
            (k2, 0, 128 - 48, 48), (q2, 64, 0, 48),
            (k3, 0, 128 - 16, 16), (q3, 96, 0, 16),
        ]
    ):
        ref[pl.ds(at_row, size), :] = columns(meta_in[i, pl.ds(4, 1), :])[top : top + size]
    received(halo[1])
    shift = 8 * (cap // 8 - c_live)
    index = rows_of(half, more)
    limit = live + jnp.where(has_next, right, 0)
    late = pl.ds(left + half, more)
    old = index < live
    new = index < limit
    late_a = jnp.where(
        new, jnp.where(old, wide_a[late, :], a_high[pl.ds(shift, more), :]), 0.0
    )
    wide_a[late, :] = late_a
    wide_j[late, :] = jnp.where(new, 1.0 / (jnp.where(new, late_a, 16.0) + diag), 0.0)
    wide_b[late, :] = jnp.where(
        new, jnp.where(old, wide_b[late, :], ghost_high[pl.ds(shift, more), :]), 0.0
    )

    n2 = lax.div(count(at(-2)), 8)
    p1 = lax.div(count(at(1)), 8)
    p2 = lax.div(count(at(2)), 8)
    e2 = base - n1
    e3 = e2 - n2
    s1 = base + c_live
    s2 = s1 + p1
    s3 = s2 + p2
    reach = c_cap + edge
    c_low = jnp.maximum(
        base - reach, jnp.where(me >= 3, 0, jnp.where(me == 2, e3, jnp.where(me == 1, e2, base)))
    )
    c_high = jnp.minimum(
        s1 + reach,
        jnp.where(
            me + 3 < n, s3 + reach,
            jnp.where(me + 3 == n, s3, jnp.where(me + 2 == n, s2, s1)),
        ),
    )

    def zeros(rows):
        return jnp.zeros((rows, 128), F32)

    r = rows_of(0, base)
    v2 = jnp.concatenate([k2[pl.ds(48 - e2, 48), :], zeros(base - 48)], 0)
    v3 = jnp.concatenate([k3[pl.ds(16 - e3, 16), :], zeros(base - 16)], 0)
    value = jnp.where(r >= e2, k1[pl.ds(0, base), :], jnp.where(r >= e3, v2, v3))
    c_a[pl.ds(0, base), :] = jnp.where(r >= c_low, value, 0.0)
    r = rows_of(base, c_cap + base)
    v0 = jnp.concatenate([mean, zeros(base)], 0)
    v1 = jnp.concatenate([zeros(32), q1[pl.ds(c_cap - c_live, 112), :]], 0)
    v2 = jnp.concatenate([zeros(64), q2[pl.ds(208 - s2, 80), :]], 0)
    v3 = jnp.concatenate([zeros(96), q3[pl.ds(272 - s3, 48), :]], 0)
    value = jnp.where(r < s1, v0, jnp.where(r < s2, v1, jnp.where(r < s3, v2, v3)))
    c_a[pl.ds(base, c_cap + base), :] = jnp.where(r < c_high, value, 0.0)
    r = rows_of(0, c_total)
    c_live_rows = (r >= c_low) & (r < c_high)
    c_j[...] = jnp.where(
        c_live_rows, 1.0 / (jnp.where(c_live_rows, c_a[...], 16.0) + diag), 0.0
    )

    for c in (coarse[1], coarse[3], coarse[4]):
        received(c)
    o1 = s1 - edge
    o2 = s2 - edge
    o3 = s3 - edge
    t1 = jnp.where(me == n - 1, c_total, o1)
    t2 = jnp.where(me == n - 2, c_total, o2)
    t3 = jnp.where(me == n - 3, c_total, o3)
    f2 = e2 - edge
    r = rows_of(front, c_total - front)
    v0 = jnp.concatenate([c_own[pl.ds(front + 4, base), :], zeros(front)], 0)
    v1 = jnp.concatenate([zeros(24), r1[pl.ds(136 - o1, 128), :]], 0)
    v2 = jnp.concatenate([zeros(56), r2[pl.ds(200 - o2, 96), :]], 0)
    v3 = jnp.concatenate([zeros(88), r3[pl.ds(264 - o3, 64), :]], 0)
    value = jnp.where(r < t1, v0, jnp.where(r < t2, v1, jnp.where(r < t3, v2, v3)))
    c_b[pl.ds(front, c_total - front), :] = jnp.where(
        (r >= c_low) & (r < c_high), value, 0.0
    )
    for c in (coarse[2], coarse[0]):
        received(c)
    r = rows_of(0, front)
    v1 = l1[pl.ds(4, front), :]
    v2 = jnp.concatenate([l2[pl.ds(40 - f2, 40), :], zeros(front - 40)], 0)
    value = jnp.where(
        r >= base - edge, c_own[pl.ds(4, front), :], jnp.where(r >= f2, v1, v2)
    )
    c_b[pl.ds(0, front), :] = jnp.where(r >= c_low, value, 0.0)
    first = c_j[...] * c_b[...] * (1.0 / CENTER)
    c_x[pl.ds(0, c_total), :] = first
    c_d[...] = first
    for i, (keep, gain) in enumerate(pairs):
        low = stride * (i + 1)
        improve(c_x, c_d, c_a, c_j, c_b, low, c_total - low, keep, gain)

    received(halo_x)
    index = rows_of(left, cap + right - left)
    keep_x = live - jnp.where(has_next, 2 * stride, 0)
    late = pl.ds(2 * left, cap + right - left)
    x[late, :] = jnp.where(
        index < limit,
        jnp.where(index < keep_x, x[late, :], x_high[pl.ds(shift, cap + right - left), :]),
        0.0,
    )
    rows = c_cap + 2 * edge
    hi, lo = split(c_x[pl.ds(base - edge, rows), :])
    pair = jnp.concatenate([hi, lo], 1)
    for begin in range(0, 1024, 256):
        part = jnp.dot(
            pair, pro_w[:, pl.ds(begin, 256)], preferred_element_type=F32
        ) + jnp.dot(hi, pro_low[:, pl.ds(begin, 256)], preferred_element_type=F32)
        for k in range(2):
            where = pl.ds(right + begin // 128 + k, rows, stride=8)
            x[where, :] = x[where, :] + part[:, 128 * k : 128 * k + 128]

    low, high = left - 2 * stride, total - stride
    improve(x, d, wide_a, wide_j, wide_b, low, high, None, 1.0 / CENTER)
    for keep, gain in pairs:
        low, high = low + stride, high - stride
        improve(x, d, wide_a, wide_j, wide_b, low, high, keep, gain)
    out_ref[...] = jnp.where(own_rows, x[own, :], 0.0)
    for c in halo + metas + coarse + [halo_x, raw]:
        sent(c)


def shards(n, lanes, right_side, cell_coef, fine_count, cell_matrix, face_near, face_far, prolong):
    cap = right_side.shape[0]
    stride = cap // 16
    left = 6 * stride
    right = 3 * stride
    total = left + cap + right
    c_cap = cap // 8
    base = c_cap + 16
    c_total = 2 * base + c_cap
    half = cap // 2

    def vmem(*shape, dtype=F32):
        return pltpu.VMEM(shape, dtype)

    scratch = [
        pltpu.SMEM(fine_count.shape, jnp.int32), vmem(cap, 128), vmem(4, 128),
        vmem(128, 128), vmem(128, 128), vmem(128, 128), vmem(8, 128, 128),
        vmem(left, 128), vmem(left, 128), vmem(cap + right, 128), vmem(8, 128),
        vmem(6, 8, 128), vmem(4, 128),
        vmem(cap, 128), vmem(cap + right, 128), vmem(total, 128), vmem(total, 128),
        vmem(total, 128), vmem(total + stride, 128), vmem(total, 128),
        vmem(5, total + 2 * stride, 128), vmem(cap + right + stride + 8, 128),
        vmem(9 * stride, 128), vmem(9 * stride, 128), vmem(9 * stride, 128),
        vmem(8 * stride, 128),
        vmem(256, 768, dtype=BF16), vmem(256, 256, dtype=BF16),
        vmem(2048, 256, dtype=BF16),
        vmem(256, 1024, dtype=BF16), vmem(128, 1024, dtype=BF16),
        vmem(168, 128), vmem(c_cap, 128), vmem(2 * c_cap + 8, 128),
        vmem(88, 128), vmem(80, 128), vmem(168, 128), vmem(168, 128), vmem(168, 128),
    ]
    scratch += [vmem(base + 8, 128)] * 3 + [vmem(base + c_cap + 8, 128)] * 3
    scratch += [vmem(c_total, 128)] * 3 + [vmem(c_total + stride, 128), vmem(c_total, 128)]
    scratch += [vmem(5 * stride, 128), vmem(half + 416, 128)]
    dma = pltpu.SemaphoreType.DMA
    scratch += [dma((7,)), dma((3,)), dma((3,)), dma((6,)), dma((6,)), dma((5,)), dma((5,))]
    scratch += [dma((1,)), dma((1,))]
    return pl.pallas_call(
        functools.partial(cycle, n, lanes, cap),
        out_shape=jax.ShapeDtypeStruct(right_side.shape, F32),
        in_specs=[pl.BlockSpec(memory_space=pltpu.MemorySpace.HBM)] * 7,
        out_specs=pl.BlockSpec(memory_space=pltpu.VMEM),
        scratch_shapes=scratch,
        compiler_params=pltpu.CompilerParams(
            collective_id=0, has_side_effects=True, vmem_limit_bytes=32 * 2**20
        ),
        name="cycle",
    )(
        *(
            pltpu.with_memory_space_constraint(v, pltpu.MemorySpace.HBM)
            for v in (
                fine_count, right_side, cell_coef.reshape(4, 128), cell_matrix, face_near,
                face_far, prolong,
            )
        )
    )


def solution(mesh):
    placed = (P(("sfc", "lvl"), None), P(("sfc", "lvl")), P(), P(), P(), P(), P())
    lanes = mesh.shape["lvl"]
    n = mesh.shape["sfc"] * lanes
    return jax.shard_map(
        functools.partial(shards, n, lanes),
        mesh=mesh, in_specs=placed, out_specs=P(("sfc", "lvl"), None), check_vma=False,
    )
```
